32 devices in a mesh: sector: 16 (over z, y, x), block: 2 (over core).
Axes of the slice: x: 2, y: 2, z: 4, core: 2. Of those that a mesh axis runs over, the one named last changes fastest.
Arguments:
- adjoint_prev: float32 [5, 16, 128, 128], P(None, 'block', 'sector'), may hold values from -6 to 6
- adjoint_source: float32 [5, 16, 128, 128], P(None, 'block', 'sector'), may hold values from -6 to 6
- face_matrices: bfloat16 [3, 5, 5, 16, 128, 128], P(None, None, None, 'block', 'sector'), may hold values from -2.5 to 2.5
- inverse_blocks: bfloat16 [5, 5, 16, 128, 128], P(None, None, 'block', 'sector')
- sector_offset: int32 [1], replicated, may hold values from 1 to 15
- donor_cells: int32 [128], P('sector'), may hold values from 0 to 7
- donor_weights: float32 [128], P('sector'), may hold values from 0.1 to 0.9
Outputs:
- adjoint: float32 [5, 16, 128, 128], P(None, 'block', 'sector')
- last_update: float32 [5, 16, 128, 128], P(None, 'block', 'sector')
The draws below stay inside these ranges and needn't reach their ends.
All inputs are finite; a program needn't handle non-finite values.
Results may differ from the reference program's by a relative error of at most 0.0003.
Values sent between devices are 32-bit elements; how exact they have to be, the bound alone decides.
A program may use at most 64 MiB of HBM per device.

```python
import jax
import jax.numpy as jnp

CT = 8
NRAD = 128
ITERS = 4
NAX = 16
NCIRC = 128
N_SECTOR = 16


def draw_inverse_blocks(key, part):
    key_off = jax.random.fold_in(key, 11)
    key_diag = jax.random.fold_in(key, 12)
    off_part = 0.06 * jax.random.normal(key_off, (5, 5, NAX, NCIRC, NRAD), jnp.float32)
    diag_part = jnp.exp(jax.random.uniform(key_diag, (5, NAX, NCIRC, NRAD), jnp.float32, jnp.log(0.15), jnp.log(0.3)))
    identity = jnp.eye(5, dtype=jnp.float32)[:, :, None, None, None]
    return (off_part * (1.0 - identity) + identity * diag_part[:, None]).astype(jnp.bfloat16)


def touch_ends(values, key, least, largest):
    longest = values.shape.index(max(values.shape))
    spots = []
    for shift in (0, 1):
        where = [jax.random.randint(jax.random.fold_in(key, axis), (), 0, length) for axis, length in enumerate(values.shape)]
        where[longest] = (where[longest] + shift) % values.shape[longest]
        spots.append(tuple(where))
    return values.at[spots[0]].set(least).at[spots[1]].set(largest)


def block_scale(rng, shape, pieces, low, largest):
    loudness = 1.0
    for dim, blocks in pieces:
        steps = jax.random.uniform(jax.random.fold_in(jax.random.fold_in(rng, 6), dim), (blocks,), jnp.float32, low / len(pieces), largest / len(pieces))
        loudness = loudness * jnp.repeat(jnp.exp(steps), shape[dim] // blocks).reshape((-1,) + (1,) * (len(shape) - 1 - dim))
    return loudness


def scatter_about(key, extent, deviation, reach, shards=(), kind=jnp.bfloat16):
    factor_of = block_scale(key, extent, shards, -0.22, 0.18) if shards else 1.0
    array = jax.random.normal(key, extent, jnp.float32) * deviation * factor_of
    return jnp.minimum(jnp.maximum(array, -reach), reach).astype(kind)


def setup_inputs(seed: int = 0) -> dict:
    streams_of = jax.random.split(jax.random.key(seed), 8)
    return {
        "adjoint_prev": scatter_about(streams_of[0], (5, NAX, NCIRC, NRAD), 1.0, 6.0, ((1, 2), (2, 16)), jnp.float32),
        "adjoint_source": scatter_about(streams_of[1], (5, NAX, NCIRC, NRAD), 1.0, 6.0, ((1, 2), (2, 16)), jnp.float32),
        "face_matrices": scatter_about(streams_of[2], (3, 5, 5, NAX, NCIRC, NRAD), 5 ** -0.5, 2.5, ((3, 2), (4, 16))),
        "inverse_blocks": draw_inverse_blocks(jax.random.fold_in(streams_of[7], 71), 0),
        "sector_offset": jax.random.randint(streams_of[4], (1,), 1, N_SECTOR).astype(jnp.int32),
        "donor_cells": touch_ends(jax.random.randint(streams_of[5], (NCIRC,), 0, CT), jax.random.fold_in(streams_of[5], 1), 0, CT - 1).astype(jnp.int32),
        "donor_weights": jnp.clip(0.1 + 0.79999997 * jax.random.uniform(streams_of[6], (NCIRC,), jnp.float32) ** block_scale(streams_of[6], (NCIRC,), ((0, 16),), -0.2, 0.2), 0.1, 0.9),
    }


def neighbour_terms(adjoint, sector_offset, donor_cells, donor_weights):
    first = NAX // 2
    rotor_row = adjoint[:, first - 1]
    shift_cells = sector_offset[0] * CT
    base = (jnp.arange(NCIRC, dtype=jnp.int32) // CT) * CT + donor_cells
    source_one = jnp.mod(base - shift_cells, NCIRC).astype(jnp.int32)
    source_two = jnp.mod(base + 1 - shift_cells, NCIRC).astype(jnp.int32)
    weights = donor_weights[None, :, None]
    facing = weights * jnp.take(rotor_row, source_one, axis=1) + (1.0 - weights) * jnp.take(rotor_row, source_two, axis=1)
    zero_layer = jnp.zeros_like(adjoint[:, :1])
    axial_minus = jnp.concatenate([zero_layer, adjoint[:, :-1]], axis=1)
    axial_minus = axial_minus.at[:, first].set(facing)
    axial_plus = jnp.concatenate([adjoint[:, 1:], zero_layer], axis=1)
    around_minus = jnp.roll(adjoint, 1, axis=2)
    around_plus = jnp.roll(adjoint, -1, axis=2)
    padded = jnp.pad(adjoint, ((0, 0), (0, 0), (0, 0), (1, 1)))
    radial_minus = padded[:, :, :, :-2]
    radial_plus = padded[:, :, :, 2:]
    return (0.6 * axial_minus + 0.4 * axial_plus,
            0.6 * around_minus + 0.4 * around_plus,
            0.6 * radial_minus + 0.4 * radial_plus)


def sweep(adjoint, adjoint_source, face_matrices, inverse_blocks, sector_offset, donor_cells, donor_weights):
    mixed = neighbour_terms(adjoint, sector_offset, donor_cells, donor_weights)
    coupled = jnp.zeros_like(adjoint)
    for direction in range(3):
        for comp in range(5):
            coupled = coupled + face_matrices[direction, comp].astype(jnp.float32) * mixed[direction][comp][None]
    total = adjoint_source + coupled
    result = jnp.zeros_like(adjoint)
    for comp in range(5):
        result = result + inverse_blocks[:, comp].astype(jnp.float32) * total[comp][None]
    return result


def reference(adjoint_prev, adjoint_source, face_matrices, inverse_blocks, sector_offset, donor_cells, donor_weights):
    adjoint = adjoint_prev
    last_update = jnp.zeros_like(adjoint_prev)
    for sweep_number in range(ITERS):
        result = sweep(adjoint, adjoint_source, face_matrices, inverse_blocks, sector_offset, donor_cells, donor_weights)
        last_update = result - adjoint
        adjoint = result
    return adjoint, last_update
```

```python
import functools

import jax
import jax.numpy as jnp
from jax import lax
from jax.experimental import pallas as pl
from jax.experimental.pallas import tpu as pltpu
from jax.sharding import PartitionSpec as P

ITERS = 4
LOWER, UPPER = 0.6, 0.4
MESH = pl.DeviceIdType.MESH


def low_part(sectors):
    return min(d for d in range(1, sectors + 1) if sectors % d == 0 and d * d >= sectors)


def kernel(
    sectors,
    blocks,
    layers,
    around,
    prev_ref,
    source_ref,
    face_ref,
    inverse_ref,
    offset_hbm,
    cells_hbm,
    weights_hbm,
    adjoint_ref,
    update_ref,
    offset_ref,
    cells_ref,
    weights_ref,
    field,
    source,
    face16,
    inverse16,
    face,
    inverse,
    radial,
    edge,
    halo,
    part,
    part_in,
    coef,
    coef_in,
    axial,
    rim_in,
    row_out,
    rows,
    forward,
    picked,
    cross_out,
    cross,
    cross_forward,
    cross_picked,
    blend,
    local_sem,
    edge_send,
    edge_recv,
    part_send,
    part_recv,
    coef_send,
    coef_recv,
    rim_send,
    rim_recv,
    row_send,
    row_recv,
    forward_send,
    forward_recv,
    cross_send,
    cross_recv,
    cross_forward_send,
    cross_forward_recv,
):
    comps, _, lanes = prev_ref.shape
    pairs = comps * comps
    sector = lax.axis_index("sector")
    block = lax.axis_index("block")
    first = blocks // 2
    lows = low_part(sectors)
    highs = sectors // lows
    high, low = sector // lows, sector % lows
    after, before = (sector + 1) % sectors, (sector + sectors - 1) % sectors
    is_stator_face = block == first
    is_rotor_face = block == first - 1
    has_lower = (block > 0) & (block != first)
    has_upper = (block < blocks - 1) & (block != first - 1)
    rims = (around - 1, 0)

    barrier = pltpu.get_barrier_semaphore()

    def greet(to_sector, to_block):
        pl.semaphore_signal(barrier, inc=1, device_id=(to_sector, to_block), device_id_type=MESH)

    greet(after, block)
    greet(before, block)

    @pl.when(block > 0)
    def _():
        greet(sector, block - 1)

    @pl.when(block < blocks - 1)
    def _():
        greet(sector, block + 1)

    @pl.when(is_rotor_face)
    def _():
        for step in range(highs):
            greet(((high + step) % highs) * lows + low, first)

    @pl.when(is_stator_face)
    def _():
        for step in range(highs):
            greet(((high + step) % highs) * lows + low, first - 1)
        for step in range(1, lows):
            greet(high * lows + (low + step) % lows, first)

    def plane(a):
        return pl.ds(a * around, around) if isinstance(a, int) else pl.ds(pl.multiple_of(a * around, around), around)

    def column_of(c, start=0):
        return pl.ds(start + c, layers, stride=around)

    def item(n):
        return pl.ds(n * layers, layers)

    into_field = pltpu.make_async_copy(prev_ref, field.at[0, :, pl.ds(around, layers * around)], local_sem.at[0])
    into_source = pltpu.make_async_copy(source_ref, source, local_sem.at[1])
    into_face = pltpu.make_async_copy(face_ref, face16, local_sem.at[2])
    into_inverse = pltpu.make_async_copy(inverse_ref, inverse16, local_sem.at[3])
    into_offset = pltpu.make_async_copy(offset_hbm, offset_ref, local_sem.at[4])
    into_cells = pltpu.make_async_copy(cells_hbm, cells_ref, local_sem.at[5])
    into_weights = pltpu.make_async_copy(weights_hbm, weights_ref, local_sem.at[6])
    scalars = (into_offset, into_cells, into_weights)
    for copy in (into_field,) + scalars + (into_inverse, into_face, into_source):
        copy.start()

    nothing = jnp.zeros((around, lanes), jnp.float32)
    for k in range(ITERS):
        for n in range(comps):
            field[k, n, plane(0)] = nothing
            field[k, n, plane(layers + 1)] = nothing

    for copy in scalars:
        copy.wait()
    column = lax.broadcasted_iota(jnp.int32, (around, lanes), 0)
    lane = lax.broadcasted_iota(jnp.int32, (around, lanes), 1)
    donor = jnp.zeros((around, lanes), jnp.int32)
    weight = jnp.zeros((around, lanes), jnp.float32)
    for j in range(around):
        donor = jnp.where(column == j, cells_ref[j], donor)
        weight = jnp.where(column == j, weights_ref[j], weight)
    for c in range(around + 1):
        blend[plane(c)] = jnp.where(donor == c, weight, 0.0) + jnp.where(donor + 1 == c, 1.0 - weight, 0.0)
    radial_lower = jnp.where(lane == 0, 0.0, LOWER).astype(jnp.float32)
    radial_upper = jnp.where(lane == lanes - 1, 0.0, UPPER).astype(jnp.float32)
    around_lower = jnp.where(column == 0, 0.0, LOWER).astype(jnp.float32)
    around_upper = jnp.where(column == around - 1, 0.0, UPPER).astype(jnp.float32)

    offset = offset_ref[0]
    chosen = []
    for step in range(lows):
        to = high * lows + (low + step) % lows
        base = to + 2 * sectors - offset - 1
        ahead = lax.rem(low + lows - lax.rem(base, lows), lows)
        chosen.append(lax.rem(lax.div(base + ahead, lows), highs))
    slots = [lax.rem(low + 2 * sectors - offset - 1 + j, lows) for j in range(4)]

    into_field.wait()

    def take_edges(k):
        for side in range(2):
            for n in range(comps):
                edge[k // 2, side, item(n)] = field[k, n, column_of(rims[side], around)]

    take_edges(0)

    def remote(src, dst, send, recv, to):
        return pltpu.make_async_remote_copy(
            src_ref=src, dst_ref=dst, send_sem=send, recv_sem=recv, device_id=to, device_id_type=MESH
        )

    def beside(side):
        return (before if side else after, block)

    def edge_copy(k, side):
        i = k // 2
        return remote(edge.at[i, side], halo.at[i, side], edge_send.at[i, side], edge_recv.at[i, side], beside(side))

    def part_copy(k, side):
        i = k // 2
        return remote(part.at[i, side], part_in.at[i, side], part_send.at[i, side], part_recv.at[i, side], beside(side))

    def coef_copy(side):
        return remote(coef.at[side], coef_in.at[side], coef_send.at[side], coef_recv.at[side], beside(side))

    def rim_copy(k, side):
        return remote(
            field.at[k, :, plane(1 if side else layers)],
            rim_in.at[k, side],
            rim_send.at[k, side],
            rim_recv.at[k, side],
            (sector, block - 1 if side else block + 1),
        )

    def row_source(k):
        return row_out.at[k // 2] if k % 2 else field.at[k, :, plane(layers)]

    def row_copy(k, step):
        to = (high + step) % highs
        return remote(row_source(k), rows[k].at[high], row_send.at[k, step], row_recv.at[k, step], (to * lows + low, first))

    def row_arrival(k, step):
        origin = (high + highs - step) % highs
        return remote(row_source(k), rows[k].at[origin], row_send.at[k, step], row_recv.at[k, step], (origin * lows + low, first))

    def cross_copy(step):
        to = (high + step) % highs
        return remote(cross_out, cross.at[high], cross_send.at[step], cross_recv.at[step], (to * lows + low, first))

    def cross_arrival(step):
        origin = (high + highs - step) % highs
        return remote(cross_out, cross.at[origin], cross_send.at[step], cross_recv.at[step], (origin * lows + low, first))

    def forward_copy(k, step):
        to = (high * lows + (low + step) % lows, first)
        return remote(forward.at[k, step], picked[k].at[low], forward_send.at[k, step], forward_recv.at[k, step], to)

    def forward_arrival(k, step):
        origin = (low + lows - step) % lows
        to = (high * lows + origin, first)
        return remote(forward.at[k, step], picked[k].at[origin], forward_send.at[k, step], forward_recv.at[k, step], to)

    def cross_forward_copy(step):
        to = (high * lows + (low + step) % lows, first)
        return remote(
            cross_forward.at[step], cross_picked.at[low], cross_forward_send.at[step], cross_forward_recv.at[step], to
        )

    def cross_forward_arrival(step):
        origin = (low + lows - step) % lows
        to = (high * lows + origin, first)
        return remote(
            cross_forward.at[step], cross_picked.at[origin], cross_forward_send.at[step], cross_forward_recv.at[step], to
        )

    far_first = sorted(range(highs), key=lambda step: -min(step, highs - step))

    def send_rows(k):
        for step in far_first:
            row_copy(k, step).start()

    def send_rims(k):
        @pl.when(block > 0)
        def _():
            rim_copy(k, 1).start()

        @pl.when(has_upper)
        def _():
            rim_copy(k, 0).start()

    greetings = 2 + (block > 0).astype(jnp.int32) + (block < blocks - 1).astype(jnp.int32)
    greetings += jnp.where(is_rotor_face, highs, 0) + jnp.where(is_stator_face, highs + lows - 1, 0)
    pl.semaphore_wait(barrier, greetings)

    edge_copy(0, 0).start()
    edge_copy(0, 1).start()

    @pl.when(is_rotor_face)
    def _():
        send_rows(0)

    send_rims(0)

    into_inverse.wait()

    def widen_inverse(i, carry):
        for m in range(comps):
            inverse[i, m] = inverse16[i, m].astype(jnp.float32).reshape(layers * around, lanes)
        return carry

    lax.fori_loop(0, comps, widen_inverse, 0)
    into_face.wait()

    def widen(i, carry):
        for d in range(3):
            for m in range(comps):
                face[d, i, m] = face16[d, i, m].astype(jnp.float32).reshape(layers * around, lanes)
        return carry

    lax.fori_loop(0, comps, widen, 0)

    def product(direction, where, share, store):
        inv = [[inverse[p, m, where] for m in range(comps)] for p in range(comps)]

        def body(n, carry):
            give = [share * face[direction, n, m, where] for m in range(comps)]
            for p in range(comps):
                total = inv[p][0] * give[0]
                for m in range(1, comps):
                    total = total + inv[p][m] * give[m]
                store(n * comps + p, total)
            return carry

        lax.fori_loop(0, comps, body, 0)

    for side, (a, share) in enumerate(((0, LOWER), (layers - 1, UPPER))):

        def keep(i, value):
            axial[side, pl.ds(pl.multiple_of(i * around, around), around)] = value

        product(0, plane(a), share, keep)
    for side in range(2):

        def keep(i, value):
            coef[side, pl.ds(pl.multiple_of(i * layers, layers), layers)] = value

        product(1, column_of(rims[side]), LOWER if side else UPPER, keep)
        for n in range(comps):
            coef[side, pl.ds(pairs * layers + n * comps, comps)] = axial[
                0, pl.ds(n * comps * around + rims[side], comps, stride=around)
            ]
        mixing = pairs * layers + pairs
        coef[side, pl.ds(mixing, around)] = blend[pl.ds(rims[side], around, stride=around)]
        coef[side, pl.ds(mixing + around, 1)] = blend[pl.ds(around * around + rims[side], 1)]

    into_source.wait()

    def make_radial(k):
        for n in range(comps):
            for a in range(layers):
                here = field[k, n, plane(a + 1)]
                radial[n, plane(a)] = radial_lower * pltpu.roll(here, 1, 1) + radial_upper * pltpu.roll(here, lanes - 1, 1)

    def local_part(k, a):
        acc = [source[m, plane(a)] for m in range(comps)]
        for n in range(comps):
            mix = radial[n, plane(a)]
            acc = [acc[m] + face[2, n, m, plane(a)] * mix for m in range(comps)]
        for n in range(comps):
            here = field[k, n, plane(a + 1)]
            mix = around_lower * pltpu.roll(here, 1, 0) + around_upper * pltpu.roll(here, around - 1, 0)
            acc = [acc[m] + face[1, n, m, plane(a)] * mix for m in range(comps)]
        for n in range(comps):
            mix = LOWER * field[k, n, plane(a)] + UPPER * field[k, n, plane(a + 2)]
            acc = [acc[m] + face[0, n, m, plane(a)] * mix for m in range(comps)]
        for m in range(comps):
            fresh = inverse[m, 0, plane(a)] * acc[0]
            for n in range(1, comps):
                fresh = fresh + inverse[m, n, plane(a)] * acc[n]
            if k < ITERS - 1:
                field[k + 1, m, plane(a + 1)] = fresh
            else:
                adjoint_ref[m, plane(a)] = 0.0 - fresh

    def local_parts(k, start, stop):
        def body(a, carry):
            local_part(k, a)
            return carry

        lax.fori_loop(start, stop, body, 0, unroll=UNROLL)

    def add_column(k, side, m, value):
        if k < ITERS - 1:
            where = column_of(rims[side], around)
            field[k + 1, m, where] = field[k + 1, m, where] + value
        else:
            where = column_of(rims[side])
            adjoint_ref[m, where] = adjoint_ref[m, where] - value

    def add_plane(k, a, m, value):
        if k < ITERS - 1:
            field[k + 1, m, plane(a + 1)] = field[k + 1, m, plane(a + 1)] + value
        else:
            adjoint_ref[m, plane(a)] = adjoint_ref[m, plane(a)] - value

    def halo_of(k, s):
        i = k // 2
        if k % 2 == 0:
            return [halo[i, s, item(n)] for n in range(comps)]
        own = [edge[i, 1 - s, item(n)] for n in range(comps)]
        values = []
        for m in range(comps):
            total = part_in[i, s, item(m)]
            for n in range(comps):
                total = total + coef_in[s, item(n * comps + m)] * own[n]
            values.append(total)
        return values

    def fix_sides(k):
        for side in range(2):
            given = halo_of(k, 1 - side)
            for m in range(comps):
                total = coef[side, item(m)] * given[0]
                for n in range(1, comps):
                    total = total + coef[side, item(n * comps + m)] * given[n]
                add_column(k, side, m, total)

    def fix_layer(k, upper, given):
        a = layers - 1 if upper else 0
        for m in range(comps):
            total = axial[upper, plane(m)] * given[0]
            for n in range(1, comps):
                total = total + axial[upper, plane(n * comps + m)] * given[n]
            add_plane(k, a, m, total)

    def fix_upper(k):
        rim_copy(k, 1).wait_recv()
        fix_layer(k, 1, [rim_in[k, 1, n] for n in range(comps)])

    def fix_lower(k):
        rim_copy(k, 0).wait_recv()
        fix_layer(k, 0, [rim_in[k, 0, n] for n in range(comps)])

    def relay(k):
        for step in range(highs):
            row_arrival(k, step).wait_recv()
        for step in list(range(1, lows)) + [0]:
            if step:
                forward[k, step] = rows[k][chosen[step]]
                forward_copy(k, step).start()
            else:
                picked[k][low] = rows[k][chosen[step]]

    def relay_cross():
        for step in range(highs):
            cross_arrival(step).wait_recv()
        for step in list(range(1, lows)) + [0]:
            if step:
                cross_forward[step] = cross[chosen[step]]
                cross_forward_copy(step).start()
            else:
                cross_picked[low] = cross[chosen[step]]

    def got(k, j, n, c):
        return picked[k][slots[j], n, c : c + 1, :]

    def crossing(k):
        def one(j, side, other, c):
            total = None
            for n in range(comps):
                start = side * pairs + n * comps
                term = cross_picked[slots[j], start : start + comps, :] * got(k - 1, other, n, c)
                total = term if total is None else total + term
            return total

        return one(1, 1, 0, around - 1), one(1, 0, 2, 0), one(2, 1, 1, around - 1)

    def facing_of(k, extra):
        values = []
        for n in range(comps):
            total = blend[plane(around)] * got(k, 2, n, 0)
            for c in range(around):
                total = total + blend[plane(c)] * got(k, 1, n, c)
            if extra is not None:
                begin, end, next_begin = extra
                total = total + blend[plane(0)] * begin[n : n + 1] + blend[plane(around - 1)] * end[n : n + 1]
                total = total + blend[plane(around)] * next_begin[n : n + 1]
            values.append(total)
        return values

    def complete_parts(k):
        i = k // 2
        mixing = pairs * layers + pairs
        for s in range(2):
            most, last = (0, 1) if s == 0 else (2, 3)
            ratios = coef_in[s, pl.ds(mixing, around)]
            ratio = coef_in[s, pl.ds(mixing + around, 1)]
            total = part_in[i, s, pl.ds(0, comps, stride=layers)]
            for n in range(comps):
                value = jnp.sum(ratios * picked[k][slots[most], n], axis=0, keepdims=True) + ratio * got(k, last, n, 0)
                total = total + coef_in[s, pl.ds(pairs * layers + n * comps, comps)] * value
            part_in[i, s, pl.ds(0, comps, stride=layers)] = total

    def wait_forward(k):
        for step in range(1, lows):
            forward_arrival(k, step).wait_recv()

    for side in range(2):
        coef_copy(side).start()

    @pl.when(is_rotor_face)
    def _():
        for side in range(2):
            for n in range(comps):
                cross_out[pl.ds(side * pairs + n * comps, comps)] = coef[
                    side, pl.ds(n * comps * layers + layers - 1, comps, stride=layers)
                ]
        for step in far_first:
            cross_copy(step).start()

    for k in range(ITERS):
        last = k == ITERS - 1
        even = k % 2 == 0
        make_radial(k)
        local_parts(k, 0, layers)
        if last:
            for m in range(comps):
                update_ref[m] = field[k, m, pl.ds(around, layers * around)]

        @pl.when(has_lower)
        def _():
            fix_lower(k)

        if even:

            @pl.when(block < blocks - 1)
            def _():
                fix_upper(k)

            @pl.when(is_rotor_face)
            def _():
                for n in range(comps):
                    row_out[k // 2, n] = field[k + 1, n, plane(layers)]
                send_rows(k + 1)

            for side in range(2):
                for n in range(comps):
                    part[k // 2, side, item(n)] = field[k + 1, n, column_of(rims[side], around)]
                part_copy(k, side).start()

            @pl.when(is_stator_face)
            def _():
                relay(k)

            for side in range(2):
                edge_copy(k, side).wait_recv()
            fix_sides(k)

            @pl.when(is_stator_face)
            def _():
                if k == 0:
                    relay_cross()
                relay(k + 1)
                wait_forward(k)
                fix_layer(k, 0, facing_of(k, None))

            send_rims(k + 1)
        else:

            @pl.when(is_stator_face)
            def _():
                if k == 1:
                    for step in range(1, lows):
                        cross_forward_arrival(step).wait_recv()

            for side in range(2):
                if k == 1:
                    coef_copy(side).wait_recv()
                part_copy(k, side).wait_recv()

            @pl.when(is_stator_face)
            def _():
                complete_parts(k - 1)

            fix_sides(k)

            @pl.when(block < blocks - 1)
            def _():
                fix_upper(k)

            @pl.when(is_stator_face)
            def _():
                extra = crossing(k)
                wait_forward(k)
                fix_layer(k, 0, facing_of(k, extra))

            if not last:

                @pl.when(is_rotor_face)
                def _():
                    send_rows(k + 1)

                send_rims(k + 1)
                take_edges(k + 1)
                for side in range(2):
                    edge_copy(k + 1, side).start()

    for side in range(2):
        coef_copy(side).wait_send()
        for k in (0, 2):
            edge_copy(k, side).wait_send()
            part_copy(k, side).wait_send()
    for k in range(ITERS):

        @pl.when(block > 0)
        def _():
            rim_copy(k, 1).wait_send()

        @pl.when(has_upper)
        def _():
            rim_copy(k, 0).wait_send()

        @pl.when(is_rotor_face)
        def _():
            for step in range(highs):
                row_copy(k, step).wait_send()

        @pl.when(is_stator_face)
        def _():
            for step in range(1, lows):
                forward_copy(k, step).wait_send()

    @pl.when(is_rotor_face)
    def _():
        for step in range(highs):
            cross_copy(step).wait_send()

    @pl.when(is_stator_face)
    def _():
        for step in range(1, lows):
            cross_forward_copy(step).wait_send()


UNROLL = 2


def solution(mesh):
    sectors, blocks = mesh.shape["sector"], mesh.shape["block"]
    lows = low_part(sectors)
    highs = sectors // lows

    def sweeps(prev, source, face, inverse, offset, cells, weights):
        comps, layers, around, lanes = prev.shape
        f32, dma = jnp.float32, pltpu.SemaphoreType.DMA
        flat = (comps, layers * around, lanes)
        pairs = comps * comps
        row = (comps, around, lanes)
        cross = (2 * pairs, lanes)
        sides = (2, 2, comps * layers, lanes)
        coefs = (2, pairs * layers + pairs + around + 1, lanes)
        hbm = pl.BlockSpec(memory_space=pl.ANY)
        vmem = pl.BlockSpec(memory_space=pltpu.VMEM)
        negative, previous = pl.pallas_call(
            functools.partial(kernel, sectors, blocks, layers, around),
            out_shape=(pltpu.VMEM(flat, f32),) * 2,
            in_specs=[hbm] * 7,
            out_specs=(vmem, vmem),
            scratch_shapes=[
                pltpu.SMEM(offset.shape, offset.dtype),
                pltpu.SMEM(cells.shape, cells.dtype),
                pltpu.SMEM(weights.shape, weights.dtype),
                pltpu.VMEM((ITERS, comps, (layers + 2) * around, lanes), f32),
                pltpu.VMEM(flat, f32),
                pltpu.VMEM(face.shape, face.dtype),
                pltpu.VMEM(inverse.shape, inverse.dtype),
                pltpu.VMEM((3, comps) + flat, f32),
                pltpu.VMEM((comps,) + flat, f32),
                pltpu.VMEM(flat, f32),
                pltpu.VMEM(sides, f32),
                pltpu.VMEM(sides, f32),
                pltpu.VMEM(sides, f32),
                pltpu.VMEM(sides, f32),
                pltpu.VMEM(coefs, f32),
                pltpu.VMEM(coefs, f32),
                pltpu.VMEM((2, pairs * around, lanes), f32),
                pltpu.VMEM((ITERS, 2) + row, f32),
                pltpu.VMEM((2,) + row, f32),
                [pltpu.VMEM((highs,) + row, f32)] * ITERS,
                pltpu.VMEM((ITERS, lows) + row, f32),
                [pltpu.VMEM((lows,) + row, f32)] * ITERS,
                pltpu.VMEM(cross, f32),
                pltpu.VMEM((highs,) + cross, f32),
                pltpu.VMEM((lows,) + cross, f32),
                pltpu.VMEM((lows,) + cross, f32),
                pltpu.VMEM(((around + 1) * around, lanes), f32),
                dma((7,)),
                dma((2, 2)),
                dma((2, 2)),
                dma((2, 2)),
                dma((2, 2)),
                dma((2,)),
                dma((2,)),
                dma((ITERS, 2)),
                dma((ITERS, 2)),
                dma((ITERS, highs)),
                dma((ITERS, highs)),
                dma((ITERS, lows)),
                dma((ITERS, lows)),
                dma((highs,)),
                dma((highs,)),
                dma((lows,)),
                dma((lows,)),
            ],
            compiler_params=pltpu.CompilerParams(collective_id=0, has_side_effects=True),
        )(prev.reshape(flat), source.reshape(flat), face, inverse, offset, cells, weights)
        negative, previous = negative.reshape(prev.shape), previous.reshape(prev.shape)
        return 0.0 - negative, 0.0 - negative - previous

    return jax.shard_map(
        sweeps,
        mesh=mesh,
        in_specs=(
            P(None, "block", "sector", None),
            P(None, "block", "sector", None),
            P(None, None, None, "block", "sector", None),
            P(None, None, "block", "sector", None),
            P(),
            P("sector"),
            P("sector"),
        ),
        out_specs=(P(None, "block", "sector", None), P(None, "block", "sector", None)),
        check_vma=False,
    )
```

```python
import functools

import jax
import jax.numpy as jnp
from jax import lax
from jax.experimental import pallas as pl
from jax.experimental.pallas import tpu as pltpu
from jax.sharding import PartitionSpec as P

ITERS = 4
LOWER, UPPER = 0.6, 0.4
MESH = pl.DeviceIdType.MESH


def low_part(sectors):
    return min(d for d in range(1, sectors + 1) if sectors % d == 0 and d * d >= sectors)


def kernel(
    sectors,
    blocks,
    layers,
    around,
    prev_ref,
    source_ref,
    face_ref,
    inverse_ref,
    offset_hbm,
    cells_hbm,
    weights_hbm,
    adjoint_ref,
    update_ref,
    offset_ref,
    cells_ref,
    weights_ref,
    field,
    source,
    face16,
    inverse16,
    face,
    inverse,
    radial,
    edge,
    halo,
    part,
    part_in,
    coef,
    coef_in,
    near,
    near_in,
    near_halo,
    axial,
    rim_in,
    row_out,
    rows,
    forward,
    picked,
    cross_out,
    cross,
    cross_forward,
    cross_picked,
    blend,
    local_sem,
    ready,
    edge_send,
    edge_recv,
    part_send,
    part_recv,
    coef_send,
    coef_recv,
    near_send,
    near_recv,
    rim_send,
    rim_recv,
    row_send,
    row_recv,
    forward_send,
    forward_recv,
    cross_send,
    cross_recv,
    cross_forward_send,
    cross_forward_recv,
):
    comps, _, lanes = prev_ref.shape
    pairs = comps * comps
    mixing = comps + 2 * pairs
    sector = lax.axis_index("sector")
    block = lax.axis_index("block")
    first = blocks // 2
    lows = low_part(sectors)
    highs = sectors // lows
    high, low = sector // lows, sector % lows
    after, before = (sector + 1) % sectors, (sector + sectors - 1) % sectors
    is_stator_face = block == first
    is_rotor_face = block == first - 1
    has_lower = (block > 0) & (block != first)
    has_upper = (block < blocks - 1) & (block != first - 1)
    rims = (around - 1, 0)

    barrier = pltpu.get_barrier_semaphore()

    def greet(to_sector, to_block):
        pl.semaphore_signal(barrier, inc=1, device_id=(to_sector, to_block), device_id_type=MESH)

    is_end = sector == sectors - 1
    is_start = sector == 0

    @pl.when(~is_end)
    def _():
        greet(after, block)

    greet(before, block)

    @pl.when(block > 0)
    def _():
        greet(sector, block - 1)

    @pl.when(block < blocks - 1)
    def _():
        greet(sector, block + 1)

    @pl.when(is_rotor_face)
    def _():
        for step in range(highs):
            greet(((high + step) % highs) * lows + low, first)

    @pl.when(is_stator_face)
    def _():
        for step in range(highs):
            greet(((high + step) % highs) * lows + low, first - 1)
        for step in range(1, lows):
            greet(high * lows + (low + step) % lows, first)

    def plane(a):
        return pl.ds(a * around, around) if isinstance(a, int) else pl.ds(pl.multiple_of(a * around, around), around)

    def column_of(c, start=0):
        return pl.ds(start + c, layers, stride=around)

    def item(n):
        return pl.ds(n * layers, layers)

    into_field = pltpu.make_async_copy(prev_ref, field.at[0, :, pl.ds(around, layers * around)], local_sem.at[0])
    into_source = pltpu.make_async_copy(source_ref, source, local_sem.at[1])
    into_face = pltpu.make_async_copy(face_ref, face16, local_sem.at[2])
    into_inverse = pltpu.make_async_copy(inverse_ref, inverse16, local_sem.at[3])
    into_offset = pltpu.make_async_copy(offset_hbm, offset_ref, local_sem.at[4])
    into_cells = pltpu.make_async_copy(cells_hbm, cells_ref, local_sem.at[5])
    into_weights = pltpu.make_async_copy(weights_hbm, weights_ref, local_sem.at[6])
    scalars = (into_offset, into_cells, into_weights)
    for copy in (into_field,) + scalars + (into_inverse, into_face, into_source):
        copy.start()

    greetings = 2 - is_start.astype(jnp.int32) + (block > 0).astype(jnp.int32) + (block < blocks - 1).astype(jnp.int32)
    greetings += jnp.where(is_rotor_face, highs, 0) + jnp.where(is_stator_face, highs + lows - 1, 0)

    @pl.when(is_end)
    def _():
        pl.semaphore_wait(barrier, greetings)
        pl.semaphore_signal(ready, inc=1, device_id=(after, block), device_id_type=MESH)

    nothing = jnp.zeros((around, lanes), jnp.float32)
    for k in range(ITERS):
        for n in range(comps):
            field[k, n, plane(0)] = nothing
            field[k, n, plane(layers + 1)] = nothing

    for copy in scalars:
        copy.wait()
    column = lax.broadcasted_iota(jnp.int32, (around, lanes), 0)
    lane = lax.broadcasted_iota(jnp.int32, (around, lanes), 1)
    donor = jnp.zeros((around, lanes), jnp.int32)
    weight = jnp.zeros((around, lanes), jnp.float32)
    for j in range(around):
        donor = jnp.where(column == j, cells_ref[j], donor)
        weight = jnp.where(column == j, weights_ref[j], weight)
    for c in range(around + 1):
        blend[plane(c)] = jnp.where(donor == c, weight, 0.0) + jnp.where(donor + 1 == c, 1.0 - weight, 0.0)
    radial_lower = jnp.where(lane == 0, 0.0, LOWER).astype(jnp.float32)
    radial_upper = jnp.where(lane == lanes - 1, 0.0, UPPER).astype(jnp.float32)
    around_lower = jnp.where(column == 0, 0.0, LOWER).astype(jnp.float32)
    around_upper = jnp.where(column == around - 1, 0.0, UPPER).astype(jnp.float32)

    offset = offset_ref[0]
    chosen = []
    for step in range(lows):
        to = high * lows + (low + step) % lows
        base = to + 2 * sectors - offset - 1
        ahead = lax.rem(low + lows - lax.rem(base, lows), lows)
        chosen.append(lax.rem(lax.div(base + ahead, lows), highs))
    slots = [lax.rem(low + 2 * sectors - offset - 1 + j, lows) for j in range(4)]

    into_field.wait()

    def slot_of(k):
        return (0, 2, 1)[k]

    def take_edges(k):
        for side in range(2):
            for n in range(comps):
                edge[slot_of(k), side, item(n)] = field[k, n, column_of(rims[side], around)]

    take_edges(0)

    def remote(src, dst, send, recv, to):
        return pltpu.make_async_remote_copy(
            src_ref=src, dst_ref=dst, send_sem=send, recv_sem=recv, device_id=to, device_id_type=MESH
        )

    def beside(side):
        return (before if side else after, block)

    def edge_copy(k, side):
        i = slot_of(k)
        return remote(edge.at[i, side], halo.at[i, side], edge_send.at[i, side], edge_recv.at[i, side], beside(side))

    def part_copy(k, side):
        i = k // 2
        return remote(part.at[i, side], part_in.at[i, side], part_send.at[i, side], part_recv.at[i, side], beside(side))

    def coef_copy(side):
        return remote(coef.at[side], coef_in.at[side], coef_send.at[side], coef_recv.at[side], beside(side))

    def near_copy(side):
        return remote(near.at[side], near_in.at[side], near_send.at[side], near_recv.at[side], beside(side))

    def rim_copy(k, side):
        return remote(
            field.at[k, :, plane(1 if side else layers)],
            rim_in.at[k, side],
            rim_send.at[k, side],
            rim_recv.at[k, side],
            (sector, block - 1 if side else block + 1),
        )

    def row_source(k):
        return row_out.at[k // 2] if k % 2 else field.at[k, :, plane(layers)]

    def row_copy(k, step):
        to = (high + step) % highs
        return remote(row_source(k), rows[k].at[high], row_send.at[k, step], row_recv.at[k, step], (to * lows + low, first))

    def row_arrival(k, step):
        origin = (high + highs - step) % highs
        return remote(row_source(k), rows[k].at[origin], row_send.at[k, step], row_recv.at[k, step], (origin * lows + low, first))

    def cross_copy(step):
        to = (high + step) % highs
        return remote(cross_out, cross.at[high], cross_send.at[step], cross_recv.at[step], (to * lows + low, first))

    def cross_arrival(step):
        origin = (high + highs - step) % highs
        return remote(cross_out, cross.at[origin], cross_send.at[step], cross_recv.at[step], (origin * lows + low, first))

    def forward_copy(k, step):
        to = (high * lows + (low + step) % lows, first)
        return remote(forward.at[k, step], picked[k].at[low], forward_send.at[k, step], forward_recv.at[k, step], to)

    def forward_arrival(k, step):
        origin = (low + lows - step) % lows
        to = (high * lows + origin, first)
        return remote(forward.at[k, step], picked[k].at[origin], forward_send.at[k, step], forward_recv.at[k, step], to)

    def cross_forward_copy(step):
        to = (high * lows + (low + step) % lows, first)
        return remote(
            cross_forward.at[step], cross_picked.at[low], cross_forward_send.at[step], cross_forward_recv.at[step], to
        )

    def cross_forward_arrival(step):
        origin = (low + lows - step) % lows
        to = (high * lows + origin, first)
        return remote(
            cross_forward.at[step], cross_picked.at[origin], cross_forward_send.at[step], cross_forward_recv.at[step], to
        )

    far_first = sorted(range(highs), key=lambda step: -min(step, highs - step))

    def send_rows(k):
        for step in far_first:
            row_copy(k, step).start()

    def send_rims(k):
        @pl.when(block > 0)
        def _():
            rim_copy(k, 1).start()

        @pl.when(has_upper)
        def _():
            rim_copy(k, 0).start()

    @pl.when(~is_end)
    def _():
        pl.semaphore_wait(barrier, greetings)

    edge_copy(0, 0).start()

    @pl.when(~is_start)
    def _():
        edge_copy(0, 1).start()

    @pl.when(is_rotor_face)
    def _():
        send_rows(0)

    send_rims(0)

    into_inverse.wait()

    def widen_inverse(i, carry):
        for m in range(comps):
            inverse[i, m] = inverse16[i, m].astype(jnp.float32).reshape(layers * around, lanes)
        return carry

    lax.fori_loop(0, comps, widen_inverse, 0)
    into_face.wait()

    def widen(i, carry):
        for d in range(3):
            for m in range(comps):
                face[d, i, m] = face16[d, i, m].astype(jnp.float32).reshape(layers * around, lanes)
        return carry

    lax.fori_loop(0, comps, widen, 0)

    def product(direction, where, share, store):
        inv = [[inverse[p, m, where] for m in range(comps)] for p in range(comps)]

        def body(n, carry):
            give = [share * face[direction, n, m, where] for m in range(comps)]
            for p in range(comps):
                total = inv[p][0] * give[0]
                for m in range(1, comps):
                    total = total + inv[p][m] * give[m]
                store(n * comps + p, total)
            return carry

        lax.fori_loop(0, comps, body, 0)

    for side in range(2):

        def keep(i, value):
            coef[side, pl.ds(pl.multiple_of(i * layers, layers), layers)] = value

        product(1, column_of(rims[side]), LOWER if side else UPPER, keep)

    @pl.when(is_rotor_face)
    def _():
        for side in range(2):
            for n in range(comps):
                cross_out[pl.ds(side * pairs + n * comps, comps)] = coef[
                    side, pl.ds(n * comps * layers + layers - 1, comps, stride=layers)
                ]

    for side, (a, share) in enumerate(((0, LOWER), (layers - 1, UPPER))):

        def keep(i, value):
            axial[side, pl.ds(pl.multiple_of(i * around, around), around)] = value

        product(0, plane(a), share, keep)

    @pl.when(is_stator_face)
    def _():
        for side in range(2):
            for n in range(comps):
                near[side, pl.ds(comps + n * comps, comps)] = coef[side, pl.ds(n * comps * layers, comps, stride=layers)]
                near[side, pl.ds(comps + pairs + n * comps, comps)] = axial[
                    0, pl.ds(n * comps * around + rims[side], comps, stride=around)
                ]
            near[side, pl.ds(mixing, around)] = blend[pl.ds(rims[side], around, stride=around)]
            near[side, pl.ds(mixing + around, 1)] = blend[pl.ds(around * around + rims[side], 1)]

    into_source.wait()

    def make_radial(k):
        for n in range(comps):
            for a in range(layers):
                here = field[k, n, plane(a + 1)]
                radial[n, plane(a)] = radial_lower * pltpu.roll(here, 1, 1) + radial_upper * pltpu.roll(here, lanes - 1, 1)

    def local_part(k, a):
        acc = [source[m, plane(a)] for m in range(comps)]
        for n in range(comps):
            mix = radial[n, plane(a)]
            acc = [acc[m] + face[2, n, m, plane(a)] * mix for m in range(comps)]
        for n in range(comps):
            here = field[k, n, plane(a + 1)]
            mix = around_lower * pltpu.roll(here, 1, 0) + around_upper * pltpu.roll(here, around - 1, 0)
            acc = [acc[m] + face[1, n, m, plane(a)] * mix for m in range(comps)]
        for n in range(comps):
            mix = LOWER * field[k, n, plane(a)] + UPPER * field[k, n, plane(a + 2)]
            acc = [acc[m] + face[0, n, m, plane(a)] * mix for m in range(comps)]
        for m in range(comps):
            fresh = inverse[m, 0, plane(a)] * acc[0]
            for n in range(1, comps):
                fresh = fresh + inverse[m, n, plane(a)] * acc[n]
            if k < ITERS - 1:
                field[k + 1, m, plane(a + 1)] = fresh
            else:
                adjoint_ref[m, plane(a)] = 0.0 - fresh

    def send_parts(k):
        for side in range(2):
            for n in range(comps):
                part[k // 2, side, item(n)] = field[k + 1, n, column_of(rims[side], around)]
            part_copy(k, side).start()

    def local_parts(k, start, stop):
        def body(a, carry):
            local_part(k, a)
            return carry

        lax.fori_loop(start, stop, body, 0, unroll=UNROLL)

    def add_column(k, side, m, value, skip=0):
        if k < ITERS - 1:
            where = pl.ds((1 + skip) * around + rims[side], layers - skip, stride=around)
            value = value[skip:]
            field[k + 1, m, where] = field[k + 1, m, where] + value
        else:
            where = column_of(rims[side])
            adjoint_ref[m, where] = adjoint_ref[m, where] - value

    def add_plane(k, a, m, value):
        if k < ITERS - 1:
            field[k + 1, m, plane(a + 1)] = field[k + 1, m, plane(a + 1)] + value
        else:
            adjoint_ref[m, plane(a)] = adjoint_ref[m, plane(a)] - value

    def completed(k, s):
        i = k // 2
        own = [edge[i, 1 - s, item(n)] for n in range(comps)]
        values = []
        for m in range(comps):
            total = part_in[i, s, item(m)]
            for n in range(comps):
                total = total + coef_in[s, item(n * comps + m)] * own[n]
            values.append(total)
        return values

    def received(k, s):
        return [halo[slot_of(k), s, item(n)] for n in range(comps)]

    def fix_sides(k, halo_of, skip=0):
        for side in range(2):
            given = halo_of(k, 1 - side)
            for m in range(comps):
                total = coef[side, item(m)] * given[0]
                for n in range(1, comps):
                    total = total + coef[side, item(n * comps + m)] * given[n]
                add_column(k, side, m, total, skip)

    def fix_layer(k, upper, given):
        a = layers - 1 if upper else 0
        for m in range(comps):
            total = axial[upper, plane(m)] * given[0]
            for n in range(1, comps):
                total = total + axial[upper, plane(n * comps + m)] * given[n]
            add_plane(k, a, m, total)

    def fix_upper(k):
        rim_copy(k, 1).wait_recv()
        fix_layer(k, 1, [rim_in[k, 1, n] for n in range(comps)])

    def fix_lower(k):
        rim_copy(k, 0).wait_recv()
        fix_layer(k, 0, [rim_in[k, 0, n] for n in range(comps)])

    def relay(k):
        for step in range(highs):
            row_arrival(k, step).wait_recv()
        for step in list(range(1, lows)) + [0]:
            if step:
                forward[k, step] = rows[k][chosen[step]]
                forward_copy(k, step).start()
            else:
                picked[k][low] = rows[k][chosen[step]]

    def relay_cross():
        for step in range(highs):
            cross_arrival(step).wait_recv()
        for step in list(range(1, lows)) + [0]:
            if step:
                cross_forward[step] = cross[chosen[step]]
                cross_forward_copy(step).start()
            else:
                cross_picked[low] = cross[chosen[step]]

    def got(k, j, n, c):
        return picked[k][slots[j], n, c : c + 1, :]

    def crossing(k):
        def one(j, side, other, c):
            total = None
            for n in range(comps):
                start = side * pairs + n * comps
                term = cross_picked[slots[j], start : start + comps, :] * got(k - 1, other, n, c)
                total = term if total is None else total + term
            return total

        return one(1, 1, 0, around - 1), one(1, 0, 2, 0), one(2, 1, 1, around - 1)

    def facing_of(k, extra):
        values = []
        for n in range(comps):
            total = blend[plane(around)] * got(k, 2, n, 0)
            for c in range(around):
                total = total + blend[plane(c)] * got(k, 1, n, c)
            if extra is not None:
                begin, end, next_begin = extra
                total = total + blend[plane(0)] * begin[n : n + 1] + blend[plane(around - 1)] * end[n : n + 1]
                total = total + blend[plane(around)] * next_begin[n : n + 1]
            values.append(total)
        return values

    def facing_beside(k, s):
        most, last = (0, 1) if s == 0 else (2, 3)
        ratios = near_in[s, pl.ds(mixing, around)]
        ratio = near_in[s, pl.ds(mixing + around, 1)]
        total = None
        for n in range(comps):
            value = jnp.sum(ratios * picked[k][slots[most], n], axis=0, keepdims=True) + ratio * got(k, last, n, 0)
            term = near_in[s, pl.ds(comps + pairs + n * comps, comps)] * value
            total = term if total is None else total + term
        return total

    def complete_parts(k):
        for s in range(2):
            where = pl.ds(0, comps, stride=layers)
            part_in[k // 2, s, where] = part_in[k // 2, s, where] + facing_beside(k, s)

    def complete_near():
        for s in range(2):
            total = near_in[s, pl.ds(0, comps)] + facing_beside(0, s)
            for n in range(comps):
                total = total + near_in[s, pl.ds(comps + n * comps, comps)] * edge[0, 1 - s, pl.ds(n * layers, 1)]
            near_halo[s] = total

    def fix_near():
        for side in range(2):
            total = None
            for n in range(comps):
                term = near[side, pl.ds(comps + n * comps, comps)] * near_halo[1 - side, pl.ds(n, 1)]
                total = term if total is None else total + term
            for m in range(comps):
                where = pl.ds(around + rims[side], 1)
                field[2, m, where] = field[2, m, where] + total[m : m + 1]

    def wait_forward(k):
        for step in range(1, lows):
            forward_arrival(k, step).wait_recv()

    def wait_sends():
        for side in range(2):
            coef_copy(side).wait_send()
            edge_copy(0, side).wait_send()
            edge_copy(2, side).wait_send()
            part_copy(2, side).wait_send()
        for k in range(ITERS):

            @pl.when(block > 0)
            def _():
                rim_copy(k, 1).wait_send()

            @pl.when(has_upper)
            def _():
                rim_copy(k, 0).wait_send()

        @pl.when(is_rotor_face)
        def _():
            for step in range(highs):
                cross_copy(step).wait_send()
                for k in range(ITERS):
                    row_copy(k, step).wait_send()

        @pl.when(is_stator_face)
        def _():
            for side in range(2):
                near_copy(side).wait_send()
                edge_copy(1, side).wait_send()
            for step in range(1, lows):
                cross_forward_copy(step).wait_send()
                for k in range(ITERS):
                    forward_copy(k, step).wait_send()

        @pl.when(~is_stator_face)
        def _():
            for side in range(2):
                part_copy(0, side).wait_send()

    for k in range(ITERS):
        last = k == ITERS - 1
        even = k % 2 == 0
        make_radial(k)
        local_parts(k, 0, layers)
        if last:
            for m in range(comps):
                update_ref[m] = field[k, m, pl.ds(around, layers * around)]

        @pl.when(has_lower)
        def _():
            fix_lower(k)

        if even:

            @pl.when(block < blocks - 1)
            def _():
                fix_upper(k)

            @pl.when(is_rotor_face)
            def _():
                for n in range(comps):
                    row_out[k // 2, n] = field[k + 1, n, plane(layers)]
                send_rows(k + 1)
                if k == 0:
                    for step in far_first:
                        cross_copy(step).start()

            if k == 0:

                @pl.when(is_start)
                def _():
                    pl.semaphore_wait(ready, 1)
                    edge_copy(0, 1).start()

                @pl.when(is_stator_face)
                def _():
                    for side in range(2):
                        for m in range(comps):
                            near[side, pl.ds(m, 1)] = field[1, m, pl.ds(around + rims[side], 1)]
                        near_copy(side).start()

                @pl.when(~is_stator_face)
                def _():
                    send_parts(0)
                    for side in range(2):
                        coef_copy(side).start()

            else:
                send_parts(k)

            @pl.when(is_stator_face)
            def _():
                relay(k)

            for side in range(2):
                edge_copy(k, side).wait_recv()
            fix_sides(k, received)

            @pl.when(is_stator_face)
            def _():
                if k == 0:
                    take_edges(1)
                    for side in range(2):
                        edge_copy(1, side).start()
                relay(k + 1)
                if k == 0:
                    relay_cross()
                    for side in range(2):
                        coef_copy(side).start()
                        near_copy(side).wait_recv()
                wait_forward(k)
                fix_layer(k, 0, facing_of(k, None))

            send_rims(k + 1)
        elif not last:

            @pl.when(is_stator_face)
            def _():
                complete_near()
                fix_near()
                for step in range(1, lows):
                    cross_forward_arrival(step).wait_recv()
                extra = crossing(k)

                @pl.when(block < blocks - 1)
                def _():
                    fix_upper(k)

                wait_forward(k)
                fix_layer(k, 0, facing_of(k, extra))
                rim_copy(k + 1, 1).start()
                for side in range(2):
                    edge_copy(1, side).wait_recv()
                fix_sides(k, received, 1)

            @pl.when(~is_stator_face)
            def _():
                for side in range(2):
                    part_copy(0, side).wait_recv()
                    coef_copy(side).wait_recv()
                fix_sides(k, completed)

                @pl.when(block < blocks - 1)
                def _():
                    fix_upper(k)

                @pl.when(is_rotor_face)
                def _():
                    send_rows(k + 1)

                @pl.when(block > 0)
                def _():
                    rim_copy(k + 1, 1).start()

            @pl.when(has_upper)
            def _():
                rim_copy(k + 1, 0).start()

            take_edges(k + 1)
            for side in range(2):
                edge_copy(k + 1, side).start()
        else:
            for side in range(2):
                part_copy(k, side).wait_recv()

            @pl.when(is_stator_face)
            def _():
                for side in range(2):
                    coef_copy(side).wait_recv()
                complete_parts(k - 1)

            fix_sides(k, completed)
            wait_sends()

            @pl.when(block < blocks - 1)
            def _():
                fix_upper(k)

            @pl.when(is_stator_face)
            def _():
                extra = crossing(k)
                wait_forward(k)
                fix_layer(k, 0, facing_of(k, extra))


UNROLL = 2


def solution(mesh):
    sectors, blocks = mesh.shape["sector"], mesh.shape["block"]
    lows = low_part(sectors)
    highs = sectors // lows

    def sweeps(prev, source, face, inverse, offset, cells, weights):
        comps, layers, around, lanes = prev.shape
        f32, dma = jnp.float32, pltpu.SemaphoreType.DMA
        flat = (comps, layers * around, lanes)
        pairs = comps * comps
        row = (comps, around, lanes)
        cross = (2 * pairs, lanes)
        sides = (2, comps * layers, lanes)
        near = (2, comps + 2 * pairs + around + 1, lanes)
        hbm = pl.BlockSpec(memory_space=pl.ANY)
        vmem = pl.BlockSpec(memory_space=pltpu.VMEM)
        negative, previous = pl.pallas_call(
            functools.partial(kernel, sectors, blocks, layers, around),
            out_shape=(pltpu.VMEM(flat, f32),) * 2,
            in_specs=[hbm] * 7,
            out_specs=(vmem, vmem),
            scratch_shapes=[
                pltpu.SMEM(offset.shape, offset.dtype),
                pltpu.SMEM(cells.shape, cells.dtype),
                pltpu.SMEM(weights.shape, weights.dtype),
                pltpu.VMEM((ITERS, comps, (layers + 2) * around, lanes), f32),
                pltpu.VMEM(flat, f32),
                pltpu.VMEM(face.shape, face.dtype),
                pltpu.VMEM(inverse.shape, inverse.dtype),
                pltpu.VMEM((3, comps) + flat, f32),
                pltpu.VMEM((comps,) + flat, f32),
                pltpu.VMEM(flat, f32),
                pltpu.VMEM((3,) + sides, f32),
                pltpu.VMEM((3,) + sides, f32),
                pltpu.VMEM((2,) + sides, f32),
                pltpu.VMEM((2,) + sides, f32),
                pltpu.VMEM((2, pairs * layers, lanes), f32),
                pltpu.VMEM((2, pairs * layers, lanes), f32),
                pltpu.VMEM(near, f32),
                pltpu.VMEM(near, f32),
                pltpu.VMEM((2, comps, lanes), f32),
                pltpu.VMEM((2, pairs * around, lanes), f32),
                pltpu.VMEM((ITERS, 2) + row, f32),
                pltpu.VMEM((2,) + row, f32),
                [pltpu.VMEM((highs,) + row, f32)] * ITERS,
                pltpu.VMEM((ITERS, lows) + row, f32),
                [pltpu.VMEM((lows,) + row, f32)] * ITERS,
                pltpu.VMEM(cross, f32),
                pltpu.VMEM((highs,) + cross, f32),
                pltpu.VMEM((lows,) + cross, f32),
                pltpu.VMEM((lows,) + cross, f32),
                pltpu.VMEM(((around + 1) * around, lanes), f32),
                dma((7,)),
                pltpu.SemaphoreType.REGULAR,
                dma((3, 2)),
                dma((3, 2)),
                dma((2, 2)),
                dma((2, 2)),
                dma((2,)),
                dma((2,)),
                dma((2,)),
                dma((2,)),
                dma((ITERS, 2)),
                dma((ITERS, 2)),
                dma((ITERS, highs)),
                dma((ITERS, highs)),
                dma((ITERS, lows)),
                dma((ITERS, lows)),
                dma((highs,)),
                dma((highs,)),
                dma((lows,)),
                dma((lows,)),
            ],
            compiler_params=pltpu.CompilerParams(collective_id=0, has_side_effects=True),
        )(prev.reshape(flat), source.reshape(flat), face, inverse, offset, cells, weights)
        negative, previous = negative.reshape(prev.shape), previous.reshape(prev.shape)
        return 0.0 - negative, 0.0 - negative - previous

    return jax.shard_map(
        sweeps,
        mesh=mesh,
        in_specs=(
            P(None, "block", "sector", None),
            P(None, "block", "sector", None),
            P(None, None, None, "block", "sector", None),
            P(None, None, "block", "sector", None),
            P(),
            P("sector"),
            P("sector"),
        ),
        out_specs=(P(None, "block", "sector", None), P(None, "block", "sector", None)),
        check_vma=False,
    )
```

```python
import functools

import jax
import jax.numpy as jnp
from jax import lax
from jax.experimental import pallas as pl
from jax.experimental.pallas import tpu as pltpu
from jax.sharding import PartitionSpec as P

ITERS = 4
LOWER, UPPER = 0.6, 0.4
MESH = pl.DeviceIdType.MESH


def low_part(sectors):
    return min(d for d in range(1, sectors + 1) if sectors % d == 0 and d * d >= sectors)


def kernel(
    sectors,
    blocks,
    layers,
    around,
    prev_ref,
    source_ref,
    face_ref,
    inverse_ref,
    offset_hbm,
    cells_hbm,
    weights_hbm,
    adjoint_ref,
    update_ref,
    offset_ref,
    cells_ref,
    weights_ref,
    field,
    source,
    face16,
    inverse16,
    face,
    inverse,
    radial,
    edge,
    halo,
    part,
    part_in,
    coef,
    coef_in,
    near,
    near_in,
    near_halo,
    axial,
    rim_in,
    row_out,
    rows,
    forward,
    picked,
    cross_out,
    cross,
    cross_forward,
    cross_picked,
    blend,
    local_sem,
    ready,
    edge_send,
    edge_recv,
    part_send,
    part_recv,
    coef_send,
    coef_recv,
    near_send,
    near_recv,
    rim_send,
    rim_recv,
    row_send,
    row_recv,
    forward_send,
    forward_recv,
    cross_send,
    cross_recv,
    cross_forward_send,
    cross_forward_recv,
):
    comps, _, lanes = prev_ref.shape
    pairs = comps * comps
    mixing = comps + 2 * pairs
    sector = lax.axis_index("sector")
    block = lax.axis_index("block")
    first = blocks // 2
    lows = low_part(sectors)
    highs = sectors // lows
    high, low = sector // lows, sector % lows
    after, before = (sector + 1) % sectors, (sector + sectors - 1) % sectors
    is_stator_face = block == first
    is_rotor_face = block == first - 1
    has_lower = (block > 0) & (block != first)
    has_upper = (block < blocks - 1) & (block != first - 1)
    rims = (around - 1, 0)

    barrier = pltpu.get_barrier_semaphore()

    def greet(to_sector, to_block):
        pl.semaphore_signal(barrier, inc=1, device_id=(to_sector, to_block), device_id_type=MESH)

    is_end = sector == sectors - 1
    is_start = sector == 0

    @pl.when(~is_end)
    def _():
        greet(after, block)

    greet(before, block)

    @pl.when(block > 0)
    def _():
        greet(sector, block - 1)

    @pl.when(block < blocks - 1)
    def _():
        greet(sector, block + 1)

    @pl.when(is_rotor_face)
    def _():
        for step in range(highs):
            greet(((high + step) % highs) * lows + low, first)

    @pl.when(is_stator_face)
    def _():
        for step in range(highs):
            greet(((high + step) % highs) * lows + low, first - 1)
        for step in range(1, lows):
            greet(high * lows + (low + step) % lows, first)

    def plane(a):
        return pl.ds(a * around, around) if isinstance(a, int) else pl.ds(pl.multiple_of(a * around, around), around)

    def column_of(c, start=0):
        return pl.ds(start + c, layers, stride=around)

    def item(n):
        return pl.ds(n * layers, layers)

    into_field = pltpu.make_async_copy(prev_ref, field.at[0, :, pl.ds(around, layers * around)], local_sem.at[0])
    into_source = pltpu.make_async_copy(source_ref, source, local_sem.at[1])
    into_face = pltpu.make_async_copy(face_ref, face16, local_sem.at[2])
    into_inverse = pltpu.make_async_copy(inverse_ref, inverse16, local_sem.at[3])
    into_offset = pltpu.make_async_copy(offset_hbm, offset_ref, local_sem.at[4])
    into_cells = pltpu.make_async_copy(cells_hbm, cells_ref, local_sem.at[5])
    into_weights = pltpu.make_async_copy(weights_hbm, weights_ref, local_sem.at[6])
    scalars = (into_offset, into_cells, into_weights)
    for copy in (into_field,) + scalars + (into_inverse, into_face, into_source):
        copy.start()

    greetings = 2 - is_start.astype(jnp.int32) + (block > 0).astype(jnp.int32) + (block < blocks - 1).astype(jnp.int32)
    greetings += jnp.where(is_rotor_face, highs, 0) + jnp.where(is_stator_face, highs + lows - 1, 0)

    @pl.when(is_end)
    def _():
        pl.semaphore_wait(barrier, greetings)
        pl.semaphore_signal(ready, inc=1, device_id=(after, block), device_id_type=MESH)

    nothing = jnp.zeros((around, lanes), jnp.float32)
    for k in range(ITERS):
        for n in range(comps):
            field[k, n, plane(0)] = nothing
            field[k, n, plane(layers + 1)] = nothing

    for copy in scalars:
        copy.wait()
    column = lax.broadcasted_iota(jnp.int32, (around, lanes), 0)
    lane = lax.broadcasted_iota(jnp.int32, (around, lanes), 1)
    donor = jnp.zeros((around, lanes), jnp.int32)
    weight = jnp.zeros((around, lanes), jnp.float32)
    for j in range(around):
        donor = jnp.where(column == j, cells_ref[j], donor)
        weight = jnp.where(column == j, weights_ref[j], weight)
    for c in range(around + 1):
        blend[plane(c)] = jnp.where(donor == c, weight, 0.0) + jnp.where(donor + 1 == c, 1.0 - weight, 0.0)
    radial_lower = jnp.where(lane == 0, 0.0, LOWER).astype(jnp.float32)
    radial_upper = jnp.where(lane == lanes - 1, 0.0, UPPER).astype(jnp.float32)
    around_lower = jnp.where(column == 0, 0.0, LOWER).astype(jnp.float32)
    around_upper = jnp.where(column == around - 1, 0.0, UPPER).astype(jnp.float32)

    offset = offset_ref[0]
    chosen = []
    for step in range(lows):
        to = high * lows + (low + step) % lows
        base = to + 2 * sectors - offset - 1
        ahead = lax.rem(low + lows - lax.rem(base, lows), lows)
        chosen.append(lax.rem(lax.div(base + ahead, lows), highs))
    slots = [lax.rem(low + 2 * sectors - offset - 1 + j, lows) for j in range(4)]

    into_field.wait()

    def slot_of(k):
        return (0, 2, 1)[k]

    def take_edges(k):
        for side in range(2):
            for n in range(comps):
                edge[slot_of(k), side, item(n)] = field[k, n, column_of(rims[side], around)]

    take_edges(0)

    def remote(src, dst, send, recv, to):
        return pltpu.make_async_remote_copy(
            src_ref=src, dst_ref=dst, send_sem=send, recv_sem=recv, device_id=to, device_id_type=MESH
        )

    def beside(side):
        return (before if side else after, block)

    def edge_copy(k, side):
        i = slot_of(k)
        return remote(edge.at[i, side], halo.at[i, side], edge_send.at[i], edge_recv.at[i], beside(side))

    def part_copy(k, side):
        i = k // 2
        return remote(part.at[i, side], part_in.at[i, side], part_send.at[i], part_recv.at[i], beside(side))

    def coef_copy(side):
        return remote(coef.at[side], coef_in.at[side], coef_send.at[side], coef_recv.at[side], beside(side))

    def near_copy(side):
        return remote(near.at[side], near_in.at[side], near_send, near_recv, beside(side))

    def rim_copy(k, side):
        return remote(
            field.at[k, :, plane(1 if side else layers)],
            rim_in.at[k, side],
            rim_send.at[k, 1 - side],
            rim_recv.at[k, 1 - side],
            (sector, block - 1 if side else block + 1),
        )

    def row_source(k):
        return row_out.at[k // 2] if k % 2 else field.at[k, :, plane(layers)]

    def row_copy(k, step):
        to = (high + step) % highs
        return remote(row_source(k), rows[k].at[high], row_send.at[k], row_recv.at[k], (to * lows + low, first))

    def all_rows(k):
        return remote(rows[k], rows[k], row_send.at[k], row_recv.at[k], (sector, first))

    def cross_copy(step):
        to = (high + step) % highs
        return remote(cross_out, cross.at[high], cross_send, cross_recv, (to * lows + low, first))

    def all_crosses():
        return remote(cross, cross, cross_send, cross_recv, (sector, first))

    def forward_copy(k, step):
        to = (high * lows + (low + step) % lows, first)
        return remote(forward.at[k, step], picked[k].at[low], forward_send.at[k], forward_recv.at[k], to)

    def all_forwards(k):
        part = forward.at[k, pl.ds(1, lows - 1)]
        return remote(part, part, forward_send.at[k], forward_recv.at[k], (sector, first))

    def cross_forward_copy(step):
        to = (high * lows + (low + step) % lows, first)
        return remote(
            cross_forward.at[step], cross_picked.at[low], cross_forward_send, cross_forward_recv, to
        )

    def all_cross_forwards():
        part = cross_forward.at[pl.ds(1, lows - 1)]
        return remote(part, part, cross_forward_send, cross_forward_recv, (sector, first))

    def both_edges(k):
        i = slot_of(k)
        return remote(edge.at[i], halo.at[i], edge_send.at[i], edge_recv.at[i], beside(0))

    def both_parts(k):
        i = k // 2
        return remote(part.at[i], part_in.at[i], part_send.at[i], part_recv.at[i], beside(0))

    def both_near():
        return remote(near, near_in, near_send, near_recv, beside(0))

    far_first = sorted(range(highs), key=lambda step: -min(step, highs - step))

    def send_rows(k):
        for step in far_first:
            row_copy(k, step).start()

    def send_rims(k):
        @pl.when(block > 0)
        def _():
            rim_copy(k, 1).start()

        @pl.when(has_upper)
        def _():
            rim_copy(k, 0).start()

    @pl.when(~is_end)
    def _():
        pl.semaphore_wait(barrier, greetings)

    edge_copy(0, 0).start()

    @pl.when(~is_start)
    def _():
        edge_copy(0, 1).start()

    @pl.when(is_rotor_face)
    def _():
        send_rows(0)

    send_rims(0)

    into_inverse.wait()

    def widen_inverse(i, carry):
        for m in range(comps):
            inverse[i, m] = inverse16[i, m].astype(jnp.float32).reshape(layers * around, lanes)
        return carry

    lax.fori_loop(0, comps, widen_inverse, 0)
    into_face.wait()

    def widen(i, carry):
        for d in range(3):
            for m in range(comps):
                face[d, i, m] = face16[d, i, m].astype(jnp.float32).reshape(layers * around, lanes)
        return carry

    lax.fori_loop(0, comps, widen, 0)

    def product(direction, where, share, store):
        inv = [[inverse[p, m, where] for m in range(comps)] for p in range(comps)]

        def body(n, carry):
            give = [share * face[direction, n, m, where] for m in range(comps)]
            for p in range(comps):
                total = inv[p][0] * give[0]
                for m in range(1, comps):
                    total = total + inv[p][m] * give[m]
                store(n * comps + p, total)
            return carry

        lax.fori_loop(0, comps, body, 0)

    for side in range(2):

        def keep(i, value):
            coef[side, pl.ds(pl.multiple_of(i * layers, layers), layers)] = value

        product(1, column_of(rims[side]), LOWER if side else UPPER, keep)

    @pl.when(is_rotor_face)
    def _():
        for side in range(2):
            for n in range(comps):
                cross_out[pl.ds(side * pairs + n * comps, comps)] = coef[
                    side, pl.ds(n * comps * layers + layers - 1, comps, stride=layers)
                ]
        for step in far_first:
            cross_copy(step).start()

    for side, (a, share) in enumerate(((0, LOWER), (layers - 1, UPPER))):

        def keep(i, value):
            axial[side, pl.ds(pl.multiple_of(i * around, around), around)] = value

        product(0, plane(a), share, keep)

    @pl.when(is_stator_face)
    def _():
        for side in range(2):
            for n in range(comps):
                near[side, pl.ds(comps + n * comps, comps)] = coef[side, pl.ds(n * comps * layers, comps, stride=layers)]
                near[side, pl.ds(comps + pairs + n * comps, comps)] = axial[
                    0, pl.ds(n * comps * around + rims[side], comps, stride=around)
                ]
            near[side, pl.ds(mixing, around)] = blend[pl.ds(rims[side], around, stride=around)]
            near[side, pl.ds(mixing + around, 1)] = blend[pl.ds(around * around + rims[side], 1)]

    into_source.wait()

    def make_radial(k):
        for n in range(comps):
            for a in range(layers):
                here = field[k, n, plane(a + 1)]
                radial[n, plane(a)] = radial_lower * pltpu.roll(here, 1, 1) + radial_upper * pltpu.roll(here, lanes - 1, 1)

    def local_part(k, a):
        acc = [source[m, plane(a)] for m in range(comps)]
        for n in range(comps):
            mix = radial[n, plane(a)]
            acc = [acc[m] + face[2, n, m, plane(a)] * mix for m in range(comps)]
        for n in range(comps):
            here = field[k, n, plane(a + 1)]
            mix = around_lower * pltpu.roll(here, 1, 0) + around_upper * pltpu.roll(here, around - 1, 0)
            acc = [acc[m] + face[1, n, m, plane(a)] * mix for m in range(comps)]
        for n in range(comps):
            mix = LOWER * field[k, n, plane(a)] + UPPER * field[k, n, plane(a + 2)]
            acc = [acc[m] + face[0, n, m, plane(a)] * mix for m in range(comps)]
        for m in range(comps):
            fresh = inverse[m, 0, plane(a)] * acc[0]
            for n in range(1, comps):
                fresh = fresh + inverse[m, n, plane(a)] * acc[n]
            if k < ITERS - 1:
                field[k + 1, m, plane(a + 1)] = fresh
            else:
                adjoint_ref[m, plane(a)] = 0.0 - fresh

    def send_parts(k):
        for side in range(2):
            for n in range(comps):
                part[k // 2, side, item(n)] = field[k + 1, n, column_of(rims[side], around)]
            part_copy(k, side).start()

    def local_parts(k, start, stop):
        def body(a, carry):
            local_part(k, a)
            return carry

        lax.fori_loop(start, stop, body, 0, unroll=UNROLL)

    def add_column(k, side, m, value, skip=0):
        if k < ITERS - 1:
            where = pl.ds((1 + skip) * around + rims[side], layers - skip, stride=around)
            value = value[skip:]
            field[k + 1, m, where] = field[k + 1, m, where] + value
        else:
            where = column_of(rims[side])
            adjoint_ref[m, where] = adjoint_ref[m, where] - value

    def add_plane(k, a, m, value):
        if k < ITERS - 1:
            field[k + 1, m, plane(a + 1)] = field[k + 1, m, plane(a + 1)] + value
        else:
            adjoint_ref[m, plane(a)] = adjoint_ref[m, plane(a)] - value

    def completed(k, s):
        i = k // 2
        own = [edge[i, 1 - s, item(n)] for n in range(comps)]
        values = []
        for m in range(comps):
            total = part_in[i, s, item(m)]
            for n in range(comps):
                total = total + coef_in[s, item(n * comps + m)] * own[n]
            values.append(total)
        return values

    def received(k, s):
        return [halo[slot_of(k), s, item(n)] for n in range(comps)]

    def fix_sides(k, halo_of, skip=0):
        for side in range(2):
            given = halo_of(k, 1 - side)
            for m in range(comps):
                total = coef[side, item(m)] * given[0]
                for n in range(1, comps):
                    total = total + coef[side, item(n * comps + m)] * given[n]
                add_column(k, side, m, total, skip)

    def fix_layer(k, upper, given):
        a = layers - 1 if upper else 0
        for m in range(comps):
            total = axial[upper, plane(m)] * given[0]
            for n in range(1, comps):
                total = total + axial[upper, plane(n * comps + m)] * given[n]
            add_plane(k, a, m, total)

    def fix_upper(k):
        rim_copy(k, 1).wait_recv()
        fix_layer(k, 1, [rim_in[k, 1, n] for n in range(comps)])

    def fix_lower(k):
        rim_copy(k, 0).wait_recv()
        fix_layer(k, 0, [rim_in[k, 0, n] for n in range(comps)])

    def relay(k):
        all_rows(k).wait_recv()
        for step in list(range(1, lows)) + [0]:
            if step:
                forward[k, step] = rows[k][chosen[step]]
                forward_copy(k, step).start()
            else:
                picked[k][low] = rows[k][chosen[step]]

    def relay_cross():
        all_crosses().wait_recv()
        for step in list(range(1, lows)) + [0]:
            if step:
                cross_forward[step] = cross[chosen[step]]
                cross_forward_copy(step).start()
            else:
                cross_picked[low] = cross[chosen[step]]

    def got(k, j, n, c):
        return picked[k][slots[j], n, c : c + 1, :]

    def crossing(k):
        def one(j, side, other, c):
            total = None
            for n in range(comps):
                start = side * pairs + n * comps
                term = cross_picked[slots[j], start : start + comps, :] * got(k - 1, other, n, c)
                total = term if total is None else total + term
            return total

        return one(1, 1, 0, around - 1), one(1, 0, 2, 0), one(2, 1, 1, around - 1)

    def facing_of(k, extra):
        values = []
        for n in range(comps):
            total = blend[plane(around)] * got(k, 2, n, 0)
            for c in range(around):
                total = total + blend[plane(c)] * got(k, 1, n, c)
            if extra is not None:
                begin, end, next_begin = extra
                total = total + blend[plane(0)] * begin[n : n + 1] + blend[plane(around - 1)] * end[n : n + 1]
                total = total + blend[plane(around)] * next_begin[n : n + 1]
            values.append(total)
        return values

    def facing_beside(k, s):
        most, last = (0, 1) if s == 0 else (2, 3)
        ratios = near_in[s, pl.ds(mixing, around)]
        ratio = near_in[s, pl.ds(mixing + around, 1)]
        total = None
        for n in range(comps):
            value = jnp.sum(ratios * picked[k][slots[most], n], axis=0, keepdims=True) + ratio * got(k, last, n, 0)
            term = near_in[s, pl.ds(comps + pairs + n * comps, comps)] * value
            total = term if total is None else total + term
        return total

    def complete_parts(k):
        for s in range(2):
            where = pl.ds(0, comps, stride=layers)
            part_in[k // 2, s, where] = part_in[k // 2, s, where] + facing_beside(k, s)

    def complete_near():
        for s in range(2):
            total = near_in[s, pl.ds(0, comps)] + facing_beside(0, s)
            for n in range(comps):
                total = total + near_in[s, pl.ds(comps + n * comps, comps)] * edge[0, 1 - s, pl.ds(n * layers, 1)]
            near_halo[s] = total

    def fix_near():
        for side in range(2):
            total = None
            for n in range(comps):
                term = near[side, pl.ds(comps + n * comps, comps)] * near_halo[1 - side, pl.ds(n, 1)]
                total = term if total is None else total + term
            for m in range(comps):
                where = pl.ds(around + rims[side], 1)
                field[2, m, where] = field[2, m, where] + total[m : m + 1]

    def wait_forward(k):
        all_forwards(k).wait_recv()

    def wait_sends():
        for side in range(2):
            coef_copy(side).wait_send()
        both_edges(0).wait_send()
        both_edges(2).wait_send()
        both_parts(2).wait_send()
        for k in range(ITERS):

            @pl.when(block > 0)
            def _():
                rim_copy(k, 1).wait_send()

            @pl.when(has_upper)
            def _():
                rim_copy(k, 0).wait_send()

        @pl.when(is_rotor_face)
        def _():
            all_crosses().wait_send()
            for k in range(ITERS):
                all_rows(k).wait_send()

        @pl.when(is_stator_face)
        def _():
            both_near().wait_send()
            both_edges(1).wait_send()
            all_cross_forwards().wait_send()
            for k in range(ITERS):
                all_forwards(k).wait_send()

        @pl.when(~is_stator_face)
        def _():
            both_parts(0).wait_send()

    for k in range(ITERS):
        last = k == ITERS - 1
        even = k % 2 == 0
        make_radial(k)
        local_parts(k, 0, layers)
        if last:
            for m in range(comps):
                update_ref[m] = field[k, m, pl.ds(around, layers * around)]

        @pl.when(has_lower)
        def _():
            fix_lower(k)

        if even:

            @pl.when(block < blocks - 1)
            def _():
                fix_upper(k)

            @pl.when(is_rotor_face)
            def _():
                for n in range(comps):
                    row_out[k // 2, n] = field[k + 1, n, plane(layers)]
                send_rows(k + 1)

            if k == 0:

                @pl.when(is_start)
                def _():
                    pl.semaphore_wait(ready, 1)
                    edge_copy(0, 1).start()

                @pl.when(is_stator_face)
                def _():
                    for side in range(2):
                        for m in range(comps):
                            near[side, pl.ds(m, 1)] = field[1, m, pl.ds(around + rims[side], 1)]
                        near_copy(side).start()

                @pl.when(~is_stator_face)
                def _():
                    send_parts(0)
                    for side in range(2):
                        coef_copy(side).start()

            else:
                send_parts(k)

            @pl.when(is_stator_face)
            def _():
                relay(k)

            both_edges(k).wait_recv()
            fix_sides(k, received)

            @pl.when(is_stator_face)
            def _():
                if k == 0:
                    take_edges(1)
                    for side in range(2):
                        edge_copy(1, side).start()
                if k == 0:
                    relay_cross()
                relay(k + 1)
                if k == 0:
                    for side in range(2):
                        coef_copy(side).start()
                    both_near().wait_recv()
                wait_forward(k)
                fix_layer(k, 0, facing_of(k, None))

            send_rims(k + 1)
        elif not last:

            @pl.when(is_stator_face)
            def _():
                complete_near()
                fix_near()
                all_cross_forwards().wait_recv()
                extra = crossing(k)

                @pl.when(block < blocks - 1)
                def _():
                    fix_upper(k)

                wait_forward(k)
                fix_layer(k, 0, facing_of(k, extra))
                rim_copy(k + 1, 1).start()
                both_edges(1).wait_recv()
                fix_sides(k, received, 1)

            @pl.when(~is_stator_face)
            def _():
                both_parts(0).wait_recv()
                for side in range(2):
                    coef_copy(side).wait_recv()
                fix_sides(k, completed)

                @pl.when(block < blocks - 1)
                def _():
                    fix_upper(k)

                @pl.when(is_rotor_face)
                def _():
                    send_rows(k + 1)

                @pl.when(block > 0)
                def _():
                    rim_copy(k + 1, 1).start()

            @pl.when(has_upper)
            def _():
                rim_copy(k + 1, 0).start()

            take_edges(k + 1)
            for side in range(2):
                edge_copy(k + 1, side).start()
        else:
            both_parts(k).wait_recv()

            @pl.when(is_stator_face)
            def _():
                for side in range(2):
                    coef_copy(side).wait_recv()
                complete_parts(k - 1)

            fix_sides(k, completed)
            wait_sends()

            @pl.when(block < blocks - 1)
            def _():
                fix_upper(k)

            @pl.when(is_stator_face)
            def _():
                extra = crossing(k)
                wait_forward(k)
                fix_layer(k, 0, facing_of(k, extra))


UNROLL = 2


def solution(mesh):
    sectors, blocks = mesh.shape["sector"], mesh.shape["block"]
    lows = low_part(sectors)
    highs = sectors // lows

    def sweeps(prev, source, face, inverse, offset, cells, weights):
        comps, layers, around, lanes = prev.shape
        f32, dma = jnp.float32, pltpu.SemaphoreType.DMA
        flat = (comps, layers * around, lanes)
        pairs = comps * comps
        row = (comps, around, lanes)
        cross = (2 * pairs, lanes)
        sides = (2, comps * layers, lanes)
        near = (2, comps + 2 * pairs + around + 1, lanes)
        hbm = pl.BlockSpec(memory_space=pl.ANY)
        vmem = pl.BlockSpec(memory_space=pltpu.VMEM)
        negative, previous = pl.pallas_call(
            functools.partial(kernel, sectors, blocks, layers, around),
            out_shape=(pltpu.VMEM(flat, f32),) * 2,
            in_specs=[hbm] * 7,
            out_specs=(vmem, vmem),
            scratch_shapes=[
                pltpu.SMEM(offset.shape, offset.dtype),
                pltpu.SMEM(cells.shape, cells.dtype),
                pltpu.SMEM(weights.shape, weights.dtype),
                pltpu.VMEM((ITERS, comps, (layers + 2) * around, lanes), f32),
                pltpu.VMEM(flat, f32),
                pltpu.VMEM(face.shape, face.dtype),
                pltpu.VMEM(inverse.shape, inverse.dtype),
                pltpu.VMEM((3, comps) + flat, f32),
                pltpu.VMEM((comps,) + flat, f32),
                pltpu.VMEM(flat, f32),
                pltpu.VMEM((3,) + sides, f32),
                pltpu.VMEM((3,) + sides, f32),
                pltpu.VMEM((2,) + sides, f32),
                pltpu.VMEM((2,) + sides, f32),
                pltpu.VMEM((2, pairs * layers, lanes), f32),
                pltpu.VMEM((2, pairs * layers, lanes), f32),
                pltpu.VMEM(near, f32),
                pltpu.VMEM(near, f32),
                pltpu.VMEM((2, comps, lanes), f32),
                pltpu.VMEM((2, pairs * around, lanes), f32),
                pltpu.VMEM((ITERS, 2) + row, f32),
                pltpu.VMEM((2,) + row, f32),
                [pltpu.VMEM((highs,) + row, f32)] * ITERS,
                pltpu.VMEM((ITERS, lows) + row, f32),
                [pltpu.VMEM((lows,) + row, f32)] * ITERS,
                pltpu.VMEM(cross, f32),
                pltpu.VMEM((highs,) + cross, f32),
                pltpu.VMEM((lows,) + cross, f32),
                pltpu.VMEM((lows,) + cross, f32),
                pltpu.VMEM(((around + 1) * around, lanes), f32),
                dma((7,)),
                pltpu.SemaphoreType.REGULAR,
                dma((3,)),
                dma((3,)),
                dma((2,)),
                dma((2,)),
                dma((2,)),
                dma((2,)),
                dma,
                dma,
                dma((ITERS, min(blocks - 1, 2))),
                dma((ITERS, min(blocks - 1, 2))),
                dma((ITERS,)),
                dma((ITERS,)),
                dma((ITERS,)),
                dma((ITERS,)),
                dma,
                dma,
                dma,
                dma,
            ],
            compiler_params=pltpu.CompilerParams(collective_id=0, has_side_effects=True),
        )(prev.reshape(flat), source.reshape(flat), face, inverse, offset, cells, weights)
        negative, previous = negative.reshape(prev.shape), previous.reshape(prev.shape)
        return 0.0 - negative, 0.0 - negative - previous

    return jax.shard_map(
        sweeps,
        mesh=mesh,
        in_specs=(
            P(None, "block", "sector", None),
            P(None, "block", "sector", None),
            P(None, None, None, "block", "sector", None),
            P(None, None, "block", "sector", None),
            P(),
            P("sector"),
            P("sector"),
        ),
        out_specs=(P(None, "block", "sector", None), P(None, "block", "sector", None)),
        check_vma=False,
    )
```

```python
import functools

import jax
import jax.numpy as jnp
from jax import lax
from jax.experimental import pallas as pl
from jax.experimental.pallas import tpu as pltpu
from jax.sharding import PartitionSpec as P

ITERS = 4
LOWER, UPPER = 0.6, 0.4
MESH = pl.DeviceIdType.MESH


def low_part(sectors):
    return min(d for d in range(1, sectors + 1) if sectors % d == 0 and d * d >= sectors)


def kernel(
    sectors,
    blocks,
    layers,
    around,
    prev_ref,
    source_ref,
    face_ref,
    inverse_ref,
    offset_hbm,
    cells_hbm,
    weights_hbm,
    adjoint_ref,
    update_ref,
    offset_ref,
    cells_ref,
    weights_ref,
    field,
    source,
    face16,
    inverse16,
    face,
    inverse,
    radial,
    edge,
    halo,
    part,
    part_in,
    coef,
    coef_in,
    near,
    near_in,
    near_halo,
    axial,
    rim_in,
    row_out,
    rows,
    forward,
    picked,
    cross_out,
    cross,
    cross_forward,
    cross_picked,
    blend,
    local_sem,
    ready,
    edge_send,
    edge_recv,
    part_send,
    part_recv,
    coef_send,
    coef_recv,
    near_send,
    near_recv,
    rim_send,
    rim_recv,
    row_send,
    row_recv,
    forward_send,
    forward_recv,
    cross_send,
    cross_recv,
    cross_forward_send,
    cross_forward_recv,
):
    comps, _, lanes = prev_ref.shape
    pairs = comps * comps
    mixing = comps + 2 * pairs
    sector = lax.axis_index("sector")
    block = lax.axis_index("block")
    first = blocks // 2
    lows = low_part(sectors)
    highs = sectors // lows
    high, low = sector // lows, sector % lows
    after, before = (sector + 1) % sectors, (sector + sectors - 1) % sectors
    is_stator_face = block == first
    is_rotor_face = block == first - 1
    has_lower = (block > 0) & (block != first)
    has_upper = (block < blocks - 1) & (block != first - 1)
    rims = (around - 1, 0)

    def partner(step):
        return low ^ step if lows & (lows - 1) == 0 else (low + step) % lows

    barrier = pltpu.get_barrier_semaphore()

    def greet(to_sector, to_block):
        pl.semaphore_signal(barrier, inc=1, device_id=(to_sector, to_block), device_id_type=MESH)

    is_end = sector == sectors - 1
    is_start = sector == 0

    @pl.when(~is_end)
    def _():
        greet(after, block)

    greet(before, block)

    @pl.when(block > 0)
    def _():
        greet(sector, block - 1)

    @pl.when(block < blocks - 1)
    def _():
        greet(sector, block + 1)

    @pl.when(is_rotor_face)
    def _():
        for step in range(highs):
            greet(((high + step) % highs) * lows + low, first)

    @pl.when(is_stator_face)
    def _():
        for step in range(highs):
            greet(((high + step) % highs) * lows + low, first - 1)
        for step in range(1, lows):
            greet(high * lows + partner(step), first)

    def plane(a):
        return pl.ds(a * around, around) if isinstance(a, int) else pl.ds(pl.multiple_of(a * around, around), around)

    def column_of(c, start=0):
        return pl.ds(start + c, layers, stride=around)

    def item(n):
        return pl.ds(n * layers, layers)

    into_field = pltpu.make_async_copy(prev_ref, field.at[0, :, pl.ds(around, layers * around)], local_sem.at[0])
    into_source = pltpu.make_async_copy(source_ref, source, local_sem.at[1])
    into_face = pltpu.make_async_copy(face_ref, face16, local_sem.at[2])
    into_inverse = pltpu.make_async_copy(inverse_ref, inverse16, local_sem.at[3])
    into_offset = pltpu.make_async_copy(offset_hbm, offset_ref, local_sem.at[4])
    into_cells = pltpu.make_async_copy(cells_hbm, cells_ref, local_sem.at[5])
    into_weights = pltpu.make_async_copy(weights_hbm, weights_ref, local_sem.at[6])
    scalars = (into_offset, into_cells, into_weights)
    for copy in (into_field,) + scalars + (into_inverse, into_face, into_source):
        copy.start()

    greetings = 2 - is_start.astype(jnp.int32) + (block > 0).astype(jnp.int32) + (block < blocks - 1).astype(jnp.int32)
    greetings += jnp.where(is_rotor_face, highs, 0) + jnp.where(is_stator_face, highs + lows - 1, 0)

    @pl.when(is_end)
    def _():
        pl.semaphore_wait(barrier, greetings)
        pl.semaphore_signal(ready, inc=1, device_id=(after, block), device_id_type=MESH)

    nothing = jnp.zeros((around, lanes), jnp.float32)
    for k in range(ITERS):
        for n in range(comps):
            field[k, n, plane(0)] = nothing
            field[k, n, plane(layers + 1)] = nothing

    for copy in scalars:
        copy.wait()
    column = lax.broadcasted_iota(jnp.int32, (around, lanes), 0)
    lane = lax.broadcasted_iota(jnp.int32, (around, lanes), 1)
    donor = jnp.zeros((around, lanes), jnp.int32)
    weight = jnp.zeros((around, lanes), jnp.float32)
    for j in range(around):
        donor = jnp.where(column == j, cells_ref[j], donor)
        weight = jnp.where(column == j, weights_ref[j], weight)
    for c in range(around + 1):
        blend[plane(c)] = jnp.where(donor == c, weight, 0.0) + jnp.where(donor + 1 == c, 1.0 - weight, 0.0)
    radial_lower = jnp.where(lane == 0, 0.0, LOWER).astype(jnp.float32)
    radial_upper = jnp.where(lane == lanes - 1, 0.0, UPPER).astype(jnp.float32)
    around_lower = jnp.where(column == 0, 0.0, LOWER).astype(jnp.float32)
    around_upper = jnp.where(column == around - 1, 0.0, UPPER).astype(jnp.float32)

    offset = offset_ref[0]
    chosen = []
    for step in range(lows):
        to = high * lows + partner(step)
        base = to + 2 * sectors - offset - 1
        ahead = lax.rem(low + lows - lax.rem(base, lows), lows)
        chosen.append(lax.rem(lax.div(base + ahead, lows), highs))
    slots = [lax.rem(low + 2 * sectors - offset - 1 + j, lows) for j in range(4)]

    into_field.wait()

    def slot_of(k):
        return (0, 2, 1)[k]

    def take_edges(k, sides=(0, 1)):
        for side in sides:
            for n in range(comps):
                edge[slot_of(k), side, item(n)] = field[k, n, column_of(rims[side], around)]

    take_edges(0)

    def remote(src, dst, send, recv, to):
        return pltpu.make_async_remote_copy(
            src_ref=src, dst_ref=dst, send_sem=send, recv_sem=recv, device_id=to, device_id_type=MESH
        )

    def beside(side):
        return (before if side else after, block)

    def edge_copy(k, side):
        i = slot_of(k)
        return remote(edge.at[i, side], halo.at[i, side], edge_send.at[i], edge_recv.at[i, side], beside(side))

    def part_copy(k, side):
        i = k // 2
        return remote(part.at[i, side], part_in.at[i, side], part_send.at[i], part_recv.at[i], beside(side))

    def coef_copy(side):
        return remote(coef.at[side], coef_in.at[side], coef_send, coef_recv, beside(side))

    def near_copy(side):
        return remote(near.at[side], near_in.at[side], near_send, near_recv, beside(side))

    def rim_copy(k, side):
        return remote(
            field.at[k, :, plane(1 if side else layers)],
            rim_in.at[k, side],
            rim_send.at[k, 1 - side],
            rim_recv.at[k, 1 - side],
            (sector, block - 1 if side else block + 1),
        )

    def row_source(k):
        return row_out.at[k // 2] if k % 2 else field.at[k, :, plane(layers)]

    def row_copy(k, step):
        to = (high + step) % highs
        return remote(row_source(k), rows[k].at[high], row_send.at[k], row_recv.at[k], (to * lows + low, first))

    def all_rows(k):
        return remote(rows[k], rows[k], row_send.at[k], row_recv.at[k], (sector, first))

    def cross_copy(step):
        to = (high + step) % highs
        return remote(cross_out, cross.at[high], cross_send, cross_recv, (to * lows + low, first))

    def all_crosses():
        return remote(cross, cross, cross_send, cross_recv, (sector, first))

    def forward_copy(k, step):
        to = (high * lows + partner(step), first)
        return remote(forward.at[k, step], picked[k].at[low], forward_send.at[k], forward_recv.at[k], to)

    def all_forwards(k):
        part = forward.at[k, pl.ds(1, lows - 1)]
        return remote(part, part, forward_send.at[k], forward_recv.at[k], (sector, first))

    def cross_forward_copy(step):
        to = (high * lows + partner(step), first)
        return remote(
            cross_forward.at[step], cross_picked.at[low], cross_forward_send, cross_forward_recv, to
        )

    def all_cross_forwards():
        part = cross_forward.at[pl.ds(1, lows - 1)]
        return remote(part, part, cross_forward_send, cross_forward_recv, (sector, first))

    def both_edges(k):
        i = slot_of(k)
        return remote(edge.at[i], halo.at[i], edge_send.at[i], edge_recv.at[i, 0], beside(0))

    def both_parts(k):
        i = k // 2
        return remote(part.at[i], part_in.at[i], part_send.at[i], part_recv.at[i], beside(0))

    def both_near():
        return remote(near, near_in, near_send, near_recv, beside(0))

    near_last = sorted(range(lows), key=lambda step: -bin(step).count("1"))
    far_first = sorted(range(highs), key=lambda step: -min(step, highs - step))

    def send_rows(k):
        for step in far_first:
            row_copy(k, step).start()

    def send_rims(k):
        @pl.when(block > 0)
        def _():
            rim_copy(k, 1).start()

        @pl.when(has_upper)
        def _():
            rim_copy(k, 0).start()

    @pl.when(~is_end)
    def _():
        pl.semaphore_wait(barrier, greetings)

    send_rims(0)

    @pl.when(is_rotor_face)
    def _():
        send_rows(0)

    edge_copy(0, 0).start()

    @pl.when(~is_start)
    def _():
        edge_copy(0, 1).start()

    into_inverse.wait()

    def widen_inverse(i, carry):
        for m in range(comps):
            inverse[i, m] = inverse16[i, m].astype(jnp.float32).reshape(layers * around, lanes)
        return carry

    lax.fori_loop(0, comps, widen_inverse, 0)
    into_face.wait()

    def widen(i, carry):
        for d in range(3):
            for m in range(comps):
                face[d, i, m] = face16[d, i, m].astype(jnp.float32).reshape(layers * around, lanes)
        return carry

    lax.fori_loop(0, comps, widen, 0)

    def product(direction, where, share, store):
        inv = [[inverse[p, m, where] for m in range(comps)] for p in range(comps)]

        def body(n, carry):
            give = [share * face[direction, n, m, where] for m in range(comps)]
            for p in range(comps):
                total = inv[p][0] * give[0]
                for m in range(1, comps):
                    total = total + inv[p][m] * give[m]
                store(n * comps + p, total)
            return carry

        lax.fori_loop(0, comps, body, 0)

    for side in range(2):

        def keep(i, value):
            coef[side, pl.ds(pl.multiple_of(i * layers, layers), layers)] = value

        product(1, column_of(rims[side]), LOWER if side else UPPER, keep)

    @pl.when(is_rotor_face)
    def _():
        for side in range(2):
            for n in range(comps):
                cross_out[pl.ds(side * pairs + n * comps, comps)] = coef[
                    side, pl.ds(n * comps * layers + layers - 1, comps, stride=layers)
                ]
        for step in far_first:
            cross_copy(step).start()

    for side, (a, share) in enumerate(((0, LOWER), (layers - 1, UPPER))):

        def keep(i, value):
            axial[side, pl.ds(pl.multiple_of(i * around, around), around)] = value

        product(0, plane(a), share, keep)

    @pl.when(is_stator_face)
    def _():
        for side in range(2):
            for n in range(comps):
                near[side, pl.ds(comps + n * comps, comps)] = coef[side, pl.ds(n * comps * layers, comps, stride=layers)]
                near[side, pl.ds(comps + pairs + n * comps, comps)] = axial[
                    0, pl.ds(n * comps * around + rims[side], comps, stride=around)
                ]
            near[side, pl.ds(mixing, around)] = blend[pl.ds(rims[side], around, stride=around)]
            near[side, pl.ds(mixing + around, 1)] = blend[pl.ds(around * around + rims[side], 1)]

    into_source.wait()

    def make_radial(k):
        for n in range(comps):
            for a in range(layers):
                here = field[k, n, plane(a + 1)]
                radial[n, plane(a)] = radial_lower * pltpu.roll(here, 1, 1) + radial_upper * pltpu.roll(here, lanes - 1, 1)

    def local_part(k, a):
        acc = [source[m, plane(a)] for m in range(comps)]
        for n in range(comps):
            mix = radial[n, plane(a)]
            acc = [acc[m] + face[2, n, m, plane(a)] * mix for m in range(comps)]
        for n in range(comps):
            here = field[k, n, plane(a + 1)]
            mix = around_lower * pltpu.roll(here, 1, 0) + around_upper * pltpu.roll(here, around - 1, 0)
            acc = [acc[m] + face[1, n, m, plane(a)] * mix for m in range(comps)]
        for n in range(comps):
            mix = LOWER * field[k, n, plane(a)] + UPPER * field[k, n, plane(a + 2)]
            acc = [acc[m] + face[0, n, m, plane(a)] * mix for m in range(comps)]
        for m in range(comps):
            fresh = inverse[m, 0, plane(a)] * acc[0]
            for n in range(1, comps):
                fresh = fresh + inverse[m, n, plane(a)] * acc[n]
            if k < ITERS - 1:
                field[k + 1, m, plane(a + 1)] = fresh
            else:
                adjoint_ref[m, plane(a)] = 0.0 - fresh

    def send_part(k, side):
        for n in range(comps):
            part[k // 2, side, item(n)] = field[k + 1, n, column_of(rims[side], around)]
        part_copy(k, side).start()

    def local_parts(k, start, stop):
        def body(a, carry):
            local_part(k, a)
            return carry

        lax.fori_loop(start, stop, body, 0, unroll=UNROLL)

    def add_column(k, side, m, value, skip=0):
        if k < ITERS - 1:
            where = pl.ds((1 + skip) * around + rims[side], layers - skip, stride=around)
            value = value[skip:]
            field[k + 1, m, where] = field[k + 1, m, where] + value
        else:
            where = column_of(rims[side])
            adjoint_ref[m, where] = adjoint_ref[m, where] - value

    def add_plane(k, a, m, value):
        if k < ITERS - 1:
            field[k + 1, m, plane(a + 1)] = field[k + 1, m, plane(a + 1)] + value
        else:
            adjoint_ref[m, plane(a)] = adjoint_ref[m, plane(a)] - value

    def completed(k, s):
        i = k // 2
        own = [edge[i, 1 - s, item(n)] for n in range(comps)]
        values = []
        for m in range(comps):
            total = part_in[i, s, item(m)]
            for n in range(comps):
                total = total + coef_in[s, item(n * comps + m)] * own[n]
            values.append(total)
        return values

    def sent(k, s):
        return [part_in[k // 2, s, item(n)] for n in range(comps)]

    def received(k, s):
        return [halo[slot_of(k), s, item(n)] for n in range(comps)]

    def fix_side(k, side, halo_of, skip=0):
        given = halo_of(k, 1 - side)
        for m in range(comps):
            total = coef[side, item(m)] * given[0]
            for n in range(1, comps):
                total = total + coef[side, item(n * comps + m)] * given[n]
            add_column(k, side, m, total, skip)

    def by_place(body):
        for parity in range(2):

            @pl.when(sector % 2 == parity)
            def _():
                body(1 - parity, parity)

    def fix_layer(k, upper, given):
        a = layers - 1 if upper else 0
        for m in range(comps):
            total = axial[upper, plane(m)] * given[0]
            for n in range(1, comps):
                total = total + axial[upper, plane(n * comps + m)] * given[n]
            add_plane(k, a, m, total)

    def fix_upper(k):
        rim_copy(k, 1).wait_recv()
        fix_layer(k, 1, [rim_in[k, 1, n] for n in range(comps)])

    def fix_lower(k):
        rim_copy(k, 0).wait_recv()
        fix_layer(k, 0, [rim_in[k, 0, n] for n in range(comps)])

    def relay(k):
        all_rows(k).wait_recv()
        for step in near_last:
            if step:
                forward[k, step] = rows[k][chosen[step]]
                forward_copy(k, step).start()
            else:
                picked[k][low] = rows[k][chosen[step]]

    def relay_cross():
        all_crosses().wait_recv()
        for step in near_last:
            if step:
                cross_forward[step] = cross[chosen[step]]
                cross_forward_copy(step).start()
            else:
                cross_picked[low] = cross[chosen[step]]

    def got(k, j, n, c):
        return picked[k][slots[j], n, c : c + 1, :]

    def crossing(k):
        def one(j, side, other, c):
            total = None
            for n in range(comps):
                start = side * pairs + n * comps
                term = cross_picked[slots[j], start : start + comps, :] * got(k - 1, other, n, c)
                total = term if total is None else total + term
            return total

        return one(1, 1, 0, around - 1), one(1, 0, 2, 0), one(2, 1, 1, around - 1)

    def facing_of(k, extra):
        values = []
        for n in range(comps):
            total = blend[plane(around)] * got(k, 2, n, 0)
            for c in range(around):
                total = total + blend[plane(c)] * got(k, 1, n, c)
            if extra is not None:
                begin, end, next_begin = extra
                total = total + blend[plane(0)] * begin[n : n + 1] + blend[plane(around - 1)] * end[n : n + 1]
                total = total + blend[plane(around)] * next_begin[n : n + 1]
            values.append(total)
        return values

    def facing_beside(k, s):
        most, last = (0, 1) if s == 0 else (2, 3)
        ratios = near_in[s, pl.ds(mixing, around)]
        ratio = near_in[s, pl.ds(mixing + around, 1)]
        total = None
        for n in range(comps):
            value = jnp.sum(ratios * picked[k][slots[most], n], axis=0, keepdims=True) + ratio * got(k, last, n, 0)
            term = near_in[s, pl.ds(comps + pairs + n * comps, comps)] * value
            total = term if total is None else total + term
        return total

    def complete_parts(k):
        for s in range(2):
            where = pl.ds(0, comps, stride=layers)
            part_in[k // 2, s, where] = part_in[k // 2, s, where] + facing_beside(k, s)

    def complete_near():
        for s in range(2):
            total = near_in[s, pl.ds(0, comps)] + facing_beside(0, s)
            for n in range(comps):
                total = total + near_in[s, pl.ds(comps + n * comps, comps)] * edge[0, 1 - s, pl.ds(n * layers, 1)]
            near_halo[s] = total

    def fix_near():
        for side in range(2):
            total = None
            for n in range(comps):
                term = near[side, pl.ds(comps + n * comps, comps)] * near_halo[1 - side, pl.ds(n, 1)]
                total = term if total is None else total + term
            for m in range(comps):
                where = pl.ds(around + rims[side], 1)
                field[2, m, where] = field[2, m, where] + total[m : m + 1]

    def wait_forward(k):
        all_forwards(k).wait_recv()

    def wait_sends():
        coef_copy(0).wait_send()
        both_edges(0).wait_send()
        both_edges(2).wait_send()
        both_parts(2).wait_send()
        for k in range(ITERS):

            @pl.when(block > 0)
            def _():
                rim_copy(k, 1).wait_send()

            @pl.when(has_upper)
            def _():
                rim_copy(k, 0).wait_send()

        @pl.when(is_rotor_face)
        def _():
            all_crosses().wait_send()
            for k in range(ITERS):
                all_rows(k).wait_send()

        @pl.when(is_stator_face)
        def _():
            both_near().wait_send()
            both_edges(1).wait_send()
            all_cross_forwards().wait_send()
            for k in range(ITERS):
                all_forwards(k).wait_send()

        @pl.when(~is_stator_face)
        def _():
            edge_copy(1, 0).wait_send()
            part_copy(0, 0).wait_send()

    def arrive(k, side):
        edge_copy(k, 1 - side).wait_recv()

    for k in range(ITERS):
        last = k == ITERS - 1
        even = k % 2 == 0
        make_radial(k)
        local_parts(k, 0, layers)
        if last:
            for m in range(comps):
                update_ref[m] = field[k, m, pl.ds(around, layers * around)]

        @pl.when(has_lower)
        def _():
            fix_lower(k)

        if even:

            @pl.when(block < blocks - 1)
            def _():
                fix_upper(k)

            @pl.when(is_rotor_face)
            def _():
                for n in range(comps):
                    row_out[k // 2, n] = field[k + 1, n, plane(layers)]
                send_rows(k + 1)

            if k == 0:

                @pl.when(is_start)
                def _():
                    pl.semaphore_wait(ready, 1)
                    edge_copy(0, 1).start()

                @pl.when(is_stator_face)
                def _():
                    for side in range(2):
                        for m in range(comps):
                            near[side, pl.ds(m, 1)] = field[1, m, pl.ds(around + rims[side], 1)]
                        near_copy(side).start()

            def begin(far, close):
                if k == 0:

                    @pl.when(~is_stator_face)
                    def _():
                        coef_copy(far).start()
                        send_part(0, far)

                else:
                    send_part(k, far)
                arrive(k, close)
                fix_side(k, close, received)
                if k == 0:
                    take_edges(1, (close,))
                    edge_copy(1, close).start()
                else:
                    send_part(k, close)

                @pl.when(is_stator_face)
                def _():
                    relay(k)

                arrive(k, far)
                fix_side(k, far, received)
                if k == 0:

                    @pl.when(is_stator_face)
                    def _():
                        take_edges(1, (far,))
                        edge_copy(1, far).start()

            by_place(begin)

            @pl.when(is_stator_face)
            def _():
                if k == 0:
                    relay_cross()
                relay(k + 1)
                if k == 0:
                    by_place(lambda far, close: coef_copy(far).start())
                    both_near().wait_recv()
                wait_forward(k)
                fix_layer(k, 0, facing_of(k, None))

            send_rims(k + 1)
        elif not last:

            @pl.when(is_stator_face)
            def _():
                complete_near()
                fix_near()
                all_cross_forwards().wait_recv()
                extra = crossing(k)

                @pl.when(block < blocks - 1)
                def _():
                    fix_upper(k)

                wait_forward(k)
                fix_layer(k, 0, facing_of(k, extra))
                rim_copy(k + 1, 1).start()
                for side in range(2):
                    arrive(1, side)
                    fix_side(k, side, received, 1)

            @pl.when(~is_stator_face)
            def _():
                def finish(far, close):
                    arrive(1, close)
                    fix_side(k, close, received)
                    part_copy(0, 1 - far).wait_recv()
                    coef_copy(1 - far).wait_recv()
                    fix_side(k, far, completed)

                by_place(finish)

                @pl.when(block < blocks - 1)
                def _():
                    fix_upper(k)

                @pl.when(is_rotor_face)
                def _():
                    send_rows(k + 1)

                @pl.when(block > 0)
                def _():
                    rim_copy(k + 1, 1).start()

            @pl.when(has_upper)
            def _():
                rim_copy(k + 1, 0).start()

            take_edges(k + 1)

            def exchange(far, close):
                edge_copy(k + 1, far).start()
                edge_copy(k + 1, close).start()

            by_place(exchange)
        else:
            both_parts(2).wait_recv()

            @pl.when(is_stator_face)
            def _():
                coef_copy(0).wait_recv()
                complete_parts(2)

            def end(far, close):
                fix_side(k, close, sent)
                fix_side(k, far, completed)

            by_place(end)
            wait_sends()

            @pl.when(block < blocks - 1)
            def _():
                fix_upper(k)

            @pl.when(is_stator_face)
            def _():
                extra = crossing(k)
                wait_forward(k)
                fix_layer(k, 0, facing_of(k, extra))


UNROLL = 2


def solution(mesh):
    sectors, blocks = mesh.shape["sector"], mesh.shape["block"]
    lows = low_part(sectors)
    highs = sectors // lows

    def sweeps(prev, source, face, inverse, offset, cells, weights):
        comps, layers, around, lanes = prev.shape
        f32, dma = jnp.float32, pltpu.SemaphoreType.DMA
        flat = (comps, layers * around, lanes)
        pairs = comps * comps
        row = (comps, around, lanes)
        cross = (2 * pairs, lanes)
        sides = (2, comps * layers, lanes)
        near = (2, comps + 2 * pairs + around + 1, lanes)
        hbm = pl.BlockSpec(memory_space=pl.ANY)
        vmem = pl.BlockSpec(memory_space=pltpu.VMEM)
        negative, previous = pl.pallas_call(
            functools.partial(kernel, sectors, blocks, layers, around),
            out_shape=(pltpu.VMEM(flat, f32),) * 2,
            in_specs=[hbm] * 7,
            out_specs=(vmem, vmem),
            scratch_shapes=[
                pltpu.SMEM(offset.shape, offset.dtype),
                pltpu.SMEM(cells.shape, cells.dtype),
                pltpu.SMEM(weights.shape, weights.dtype),
                pltpu.VMEM((ITERS, comps, (layers + 2) * around, lanes), f32),
                pltpu.VMEM(flat, f32),
                pltpu.VMEM(face.shape, face.dtype),
                pltpu.VMEM(inverse.shape, inverse.dtype),
                pltpu.VMEM((3, comps) + flat, f32),
                pltpu.VMEM((comps,) + flat, f32),
                pltpu.VMEM(flat, f32),
                pltpu.VMEM((3,) + sides, f32),
                pltpu.VMEM((3,) + sides, f32),
                pltpu.VMEM((2,) + sides, f32),
                pltpu.VMEM((2,) + sides, f32),
                pltpu.VMEM((2, pairs * layers, lanes), f32),
                pltpu.VMEM((2, pairs * layers, lanes), f32),
                pltpu.VMEM(near, f32),
                pltpu.VMEM(near, f32),
                pltpu.VMEM((2, comps, lanes), f32),
                pltpu.VMEM((2, pairs * around, lanes), f32),
                pltpu.VMEM((ITERS, 2) + row, f32),
                pltpu.VMEM((2,) + row, f32),
                [pltpu.VMEM((highs,) + row, f32)] * ITERS,
                pltpu.VMEM((ITERS, lows) + row, f32),
                [pltpu.VMEM((lows,) + row, f32)] * ITERS,
                pltpu.VMEM(cross, f32),
                pltpu.VMEM((highs,) + cross, f32),
                pltpu.VMEM((lows,) + cross, f32),
                pltpu.VMEM((lows,) + cross, f32),
                pltpu.VMEM(((around + 1) * around, lanes), f32),
                dma((7,)),
                pltpu.SemaphoreType.REGULAR,
                dma((3,)),
                dma((3, 2)),
                dma((2,)),
                dma((2,)),
                dma,
                dma,
                dma,
                dma,
                dma((ITERS, min(blocks - 1, 2))),
                dma((ITERS, min(blocks - 1, 2))),
                dma((ITERS,)),
                dma((ITERS,)),
                dma((ITERS,)),
                dma((ITERS,)),
                dma,
                dma,
                dma,
                dma,
            ],
            compiler_params=pltpu.CompilerParams(collective_id=0, has_side_effects=True),
        )(prev.reshape(flat), source.reshape(flat), face, inverse, offset, cells, weights)
        negative, previous = negative.reshape(prev.shape), previous.reshape(prev.shape)
        return 0.0 - negative, 0.0 - negative - previous

    return jax.shard_map(
        sweeps,
        mesh=mesh,
        in_specs=(
            P(None, "block", "sector", None),
            P(None, "block", "sector", None),
            P(None, None, None, "block", "sector", None),
            P(None, None, "block", "sector", None),
            P(),
            P("sector"),
            P("sector"),
        ),
        out_specs=(P(None, "block", "sector", None), P(None, "block", "sector", None)),
        check_vma=False,
    )
```

```python
import functools

import jax
import jax.numpy as jnp
from jax import lax
from jax.experimental import pallas as pl
from jax.experimental.pallas import tpu as pltpu
from jax.sharding import PartitionSpec as P

ITERS = 4
LOWER, UPPER = 0.6, 0.4
MESH = pl.DeviceIdType.MESH


def low_part(sectors):
    return min(d for d in range(1, sectors + 1) if sectors % d == 0 and d * d >= sectors)


def kernel(
    sectors,
    blocks,
    layers,
    around,
    prev_ref,
    source_ref,
    face_ref,
    inverse_ref,
    offset_hbm,
    cells_hbm,
    weights_hbm,
    adjoint_ref,
    update_ref,
    offset_ref,
    cells_ref,
    weights_ref,
    field,
    source,
    face16,
    inverse16,
    face,
    inverse,
    radial,
    edge,
    halo,
    part,
    part_in,
    coef,
    coef_in,
    near,
    near_in,
    near_halo,
    axial,
    rim_in,
    row_out,
    rows,
    forward,
    picked,
    cross_out,
    cross,
    cross_forward,
    cross_picked,
    blend,
    local_sem,
    ready,
    edge_send,
    edge_recv,
    part_send,
    part_recv,
    coef_send,
    coef_recv,
    near_send,
    near_recv,
    rim_send,
    rim_recv,
    row_send,
    row_recv,
    forward_send,
    forward_recv,
    cross_send,
    cross_recv,
    cross_forward_send,
    cross_forward_recv,
):
    comps, _, lanes = prev_ref.shape
    pairs = comps * comps
    mixing = comps + 2 * pairs
    sector = lax.axis_index("sector")
    block = lax.axis_index("block")
    first = blocks // 2
    lows = low_part(sectors)
    highs = sectors // lows
    high, low = sector // lows, sector % lows
    after, before = (sector + 1) % sectors, (sector + sectors - 1) % sectors
    is_stator_face = block == first
    is_rotor_face = block == first - 1
    has_lower = (block > 0) & (block != first)
    has_upper = (block < blocks - 1) & (block != first - 1)
    rims = (around - 1, 0)

    def partner(step):
        return low ^ step if lows & (lows - 1) == 0 else (low + step) % lows

    barrier = pltpu.get_barrier_semaphore()

    def greet(to_sector, to_block):
        pl.semaphore_signal(barrier, inc=1, device_id=(to_sector, to_block), device_id_type=MESH)

    is_end = sector == sectors - 1
    is_start = sector == 0

    @pl.when(~is_end)
    def _():
        greet(after, block)

    greet(before, block)

    @pl.when(block > 0)
    def _():
        greet(sector, block - 1)

    @pl.when(block < blocks - 1)
    def _():
        greet(sector, block + 1)

    @pl.when(is_stator_face)
    def _():
        for step in range(highs):
            greet(((high + step) % highs) * lows + low, first - 1)
        for step in range(1, lows):
            greet(high * lows + partner(step), first)

    def plane(a):
        return pl.ds(a * around, around) if isinstance(a, int) else pl.ds(pl.multiple_of(a * around, around), around)

    def column_of(c, start=0):
        return pl.ds(start + c, layers, stride=around)

    def item(n):
        return pl.ds(n * layers, layers)

    into_field = pltpu.make_async_copy(prev_ref, field.at[0, :, pl.ds(around, layers * around)], local_sem.at[0])
    into_source = pltpu.make_async_copy(source_ref, source, local_sem.at[1])
    into_face = pltpu.make_async_copy(face_ref, face16, local_sem.at[2])
    into_inverse = pltpu.make_async_copy(inverse_ref, inverse16, local_sem.at[3])
    into_offset = pltpu.make_async_copy(offset_hbm, offset_ref, local_sem.at[4])
    into_cells = pltpu.make_async_copy(cells_hbm, cells_ref, local_sem.at[5])
    into_weights = pltpu.make_async_copy(weights_hbm, weights_ref, local_sem.at[6])
    scalars = (into_offset, into_cells, into_weights)
    for copy in (into_field,) + scalars + (into_inverse, into_face, into_source):
        copy.start()

    greetings = 2 - is_start.astype(jnp.int32) + (block > 0).astype(jnp.int32) + (block < blocks - 1).astype(jnp.int32)
    greetings += jnp.where(is_rotor_face, highs, 0) + jnp.where(is_stator_face, lows - 1, 0)

    @pl.when(is_end)
    def _():
        pl.semaphore_wait(barrier, greetings)
        pl.semaphore_signal(ready, inc=1, device_id=(after, block), device_id_type=MESH)

    nothing = jnp.zeros((around, lanes), jnp.float32)
    for k in range(ITERS):
        for n in range(comps):
            field[k, n, plane(0)] = nothing
            field[k, n, plane(layers + 1)] = nothing

    for copy in scalars:
        copy.wait()
    column = lax.broadcasted_iota(jnp.int32, (around, lanes), 0)
    lane = lax.broadcasted_iota(jnp.int32, (around, lanes), 1)
    donor = jnp.zeros((around, lanes), jnp.int32)
    weight = jnp.zeros((around, lanes), jnp.float32)
    for j in range(around):
        donor = jnp.where(column == j, cells_ref[j], donor)
        weight = jnp.where(column == j, weights_ref[j], weight)
    for c in range(around + 1):
        blend[plane(c)] = jnp.where(donor == c, weight, 0.0) + jnp.where(donor + 1 == c, 1.0 - weight, 0.0)
    radial_lower = jnp.where(lane == 0, 0.0, LOWER).astype(jnp.float32)
    radial_upper = jnp.where(lane == lanes - 1, 0.0, UPPER).astype(jnp.float32)
    around_lower = jnp.where(column == 0, 0.0, LOWER).astype(jnp.float32)
    around_upper = jnp.where(column == around - 1, 0.0, UPPER).astype(jnp.float32)

    offset = offset_ref[0]
    chosen = []
    for step in range(lows):
        to = high * lows + partner(step)
        base = to + 2 * sectors - offset - 1
        ahead = lax.rem(low + lows - lax.rem(base, lows), lows)
        chosen.append(lax.rem(lax.div(base + ahead, lows), highs))
    slots = [lax.rem(low + 2 * sectors - offset - 1 + j, lows) for j in range(4)]

    into_field.wait()

    def slot_of(k):
        return (0, 2, 1)[k]

    def take_edges(k, sides=(0, 1)):
        for side in sides:
            for n in range(comps):
                edge[slot_of(k), side, item(n)] = field[k, n, column_of(rims[side], around)]

    take_edges(0)

    def remote(src, dst, send, recv, to):
        return pltpu.make_async_remote_copy(
            src_ref=src, dst_ref=dst, send_sem=send, recv_sem=recv, device_id=to, device_id_type=MESH
        )

    def beside(side):
        return (before if side else after, block)

    def edge_copy(k, side):
        i = slot_of(k)
        return remote(edge.at[i, side], halo.at[i, side], edge_send.at[i], edge_recv.at[i, side], beside(side))

    def part_copy(k, side):
        i = k // 2
        return remote(part.at[i, side], part_in.at[i, side], part_send.at[i], part_recv.at[i], beside(side))

    def coef_copy(side):
        return remote(coef.at[side], coef_in.at[side], coef_send, coef_recv, beside(side))

    def near_copy(side):
        return remote(near.at[side], near_in.at[side], near_send, near_recv, beside(side))

    def rim_copy(k, side):
        return remote(
            field.at[k, :, plane(1 if side else layers)],
            rim_in.at[k, side],
            rim_send.at[1 - side],
            rim_recv.at[k, 1 - side],
            (sector, block - 1 if side else block + 1),
        )

    def sent_rims(side):
        ours = rim_in.at[:, side]
        to = (sector, block - 1 if side else block + 1)
        return remote(ours, ours, rim_send.at[1 - side], rim_recv.at[0, 1 - side], to)

    def row_source(k):
        return row_out.at[k // 2] if k % 2 else field.at[k, :, plane(layers)]

    def row_copy(k, step):
        to = (high + step) % highs
        return remote(row_source(k), rows[k].at[high], row_send, row_recv.at[k], (to * lows + low, first))

    def all_rows(k):
        return remote(rows[k], rows[k], row_send, row_recv.at[k], (sector, first))

    def sent_rows():
        part = forward.at[:, pl.ds(0, highs)]
        return remote(part, part, row_send, row_recv.at[0], (sector, first))

    def cross_copy(step):
        to = (high + step) % highs
        return remote(cross_out, cross.at[high], cross_send, cross_recv, (to * lows + low, first))

    def all_crosses():
        return remote(cross, cross, cross_send, cross_recv, (sector, first))

    def forward_copy(k, step):
        to = (high * lows + partner(step), first)
        return remote(forward.at[k, step], picked[k].at[low], forward_send, forward_recv.at[k], to)

    def all_forwards(k):
        part = forward.at[k, pl.ds(1, lows - 1)]
        return remote(part, part, forward_send, forward_recv.at[k], (sector, first))

    def sent_forwards():
        part = forward.at[:, pl.ds(1, lows - 1)]
        return remote(part, part, forward_send, forward_recv.at[0], (sector, first))

    def cross_forward_copy(step):
        to = (high * lows + partner(step), first)
        return remote(
            cross_forward.at[step], cross_picked.at[low], cross_forward_send, cross_forward_recv, to
        )

    def all_cross_forwards():
        part = cross_forward.at[pl.ds(1, lows - 1)]
        return remote(part, part, cross_forward_send, cross_forward_recv, (sector, first))

    def both_edges(k):
        i = slot_of(k)
        return remote(edge.at[i], halo.at[i], edge_send.at[i], edge_recv.at[i, 0], beside(0))

    def both_parts(k):
        i = k // 2
        return remote(part.at[i], part_in.at[i], part_send.at[i], part_recv.at[i], beside(0))

    def both_near():
        return remote(near, near_in, near_send, near_recv, beside(0))

    near_last = sorted(range(lows), key=lambda step: -bin(step).count("1"))
    far_first = sorted(range(highs), key=lambda step: -min(step, highs - step))

    def send_rows(k):
        for step in far_first:
            row_copy(k, step).start()

    def send_rims(k):
        @pl.when(block > 0)
        def _():
            rim_copy(k, 1).start()

        @pl.when(has_upper)
        def _():
            rim_copy(k, 0).start()

    @pl.when(~is_end)
    def _():
        pl.semaphore_wait(barrier, greetings)

    send_rims(0)

    @pl.when(is_rotor_face)
    def _():
        send_rows(0)

    edge_copy(0, 0).start()

    @pl.when(~is_start)
    def _():
        edge_copy(0, 1).start()

    into_inverse.wait()

    def widen_inverse(i, carry):
        for m in range(comps):
            inverse[i, m] = inverse16[i, m].astype(jnp.float32).reshape(layers * around, lanes)
        return carry

    lax.fori_loop(0, comps, widen_inverse, 0)
    into_face.wait()

    def widen(i, carry):
        for d in range(3):
            for m in range(comps):
                face[d, i, m] = face16[d, i, m].astype(jnp.float32).reshape(layers * around, lanes)
        return carry

    lax.fori_loop(0, comps, widen, 0)

    def product(direction, where, share, store):
        inv = [[inverse[p, m, where] for m in range(comps)] for p in range(comps)]

        def body(n, carry):
            give = [share * face[direction, n, m, where] for m in range(comps)]
            for p in range(comps):
                total = inv[p][0] * give[0]
                for m in range(1, comps):
                    total = total + inv[p][m] * give[m]
                store(n * comps + p, total)
            return carry

        lax.fori_loop(0, comps, body, 0)

    for side in range(2):

        def keep(i, value):
            coef[side, pl.ds(pl.multiple_of(i * layers, layers), layers)] = value

        product(1, column_of(rims[side]), LOWER if side else UPPER, keep)

    @pl.when(is_rotor_face)
    def _():
        for side in range(2):
            for n in range(comps):
                cross_out[pl.ds(side * pairs + n * comps, comps)] = coef[
                    side, pl.ds(n * comps * layers + layers - 1, comps, stride=layers)
                ]
        for step in far_first:
            cross_copy(step).start()

    for side, (a, share) in enumerate(((0, LOWER), (layers - 1, UPPER))):

        def keep(i, value):
            axial[side, pl.ds(pl.multiple_of(i * around, around), around)] = value

        product(0, plane(a), share, keep)

    @pl.when(is_stator_face)
    def _():
        for side in range(2):
            for n in range(comps):
                near[side, pl.ds(comps + n * comps, comps)] = coef[side, pl.ds(n * comps * layers, comps, stride=layers)]
                near[side, pl.ds(comps + pairs + n * comps, comps)] = axial[
                    0, pl.ds(n * comps * around + rims[side], comps, stride=around)
                ]
            near[side, pl.ds(mixing, around)] = blend[pl.ds(rims[side], around, stride=around)]
            near[side, pl.ds(mixing + around, 1)] = blend[pl.ds(around * around + rims[side], 1)]

    into_source.wait()

    def make_radial(k):
        for n in range(comps):
            for a in range(layers):
                here = field[k, n, plane(a + 1)]
                radial[n, plane(a)] = radial_lower * pltpu.roll(here, 1, 1) + radial_upper * pltpu.roll(here, lanes - 1, 1)

    def local_part(k, a):
        acc = [source[m, plane(a)] for m in range(comps)]
        for n in range(comps):
            mix = radial[n, plane(a)]
            acc = [acc[m] + face[2, n, m, plane(a)] * mix for m in range(comps)]
        for n in range(comps):
            here = field[k, n, plane(a + 1)]
            mix = around_lower * pltpu.roll(here, 1, 0) + around_upper * pltpu.roll(here, around - 1, 0)
            acc = [acc[m] + face[1, n, m, plane(a)] * mix for m in range(comps)]
        for n in range(comps):
            mix = LOWER * field[k, n, plane(a)] + UPPER * field[k, n, plane(a + 2)]
            acc = [acc[m] + face[0, n, m, plane(a)] * mix for m in range(comps)]
        for m in range(comps):
            fresh = inverse[m, 0, plane(a)] * acc[0]
            for n in range(1, comps):
                fresh = fresh + inverse[m, n, plane(a)] * acc[n]
            if k < ITERS - 1:
                field[k + 1, m, plane(a + 1)] = fresh
            else:
                adjoint_ref[m, plane(a)] = 0.0 - fresh

    def send_part(k, side):
        for n in range(comps):
            part[k // 2, side, item(n)] = field[k + 1, n, column_of(rims[side], around)]
        part_copy(k, side).start()

    def local_parts(k, start, stop):
        def body(a, carry):
            local_part(k, a)
            return carry

        lax.fori_loop(start, stop, body, 0, unroll=UNROLL)

    def add_column(k, side, m, value, skip=0):
        if k < ITERS - 1:
            where = pl.ds((1 + skip) * around + rims[side], layers - skip, stride=around)
            value = value[skip:]
            field[k + 1, m, where] = field[k + 1, m, where] + value
        else:
            where = column_of(rims[side])
            adjoint_ref[m, where] = adjoint_ref[m, where] - value

    def add_plane(k, a, m, value):
        if k < ITERS - 1:
            field[k + 1, m, plane(a + 1)] = field[k + 1, m, plane(a + 1)] + value
        else:
            adjoint_ref[m, plane(a)] = adjoint_ref[m, plane(a)] - value

    def completed(k, s):
        i = k // 2
        own = [edge[i, 1 - s, item(n)] for n in range(comps)]
        values = []
        for m in range(comps):
            total = part_in[i, s, item(m)]
            for n in range(comps):
                total = total + coef_in[s, item(n * comps + m)] * own[n]
            values.append(total)
        return values

    def sent(k, s):
        return [part_in[k // 2, s, item(n)] for n in range(comps)]

    def received(k, s):
        return [halo[slot_of(k), s, item(n)] for n in range(comps)]

    def fix_side(k, side, halo_of, skip=0):
        given = halo_of(k, 1 - side)
        for m in range(comps):
            total = coef[side, item(m)] * given[0]
            for n in range(1, comps):
                total = total + coef[side, item(n * comps + m)] * given[n]
            add_column(k, side, m, total, skip)

    def by_place(body):
        for parity in range(2):

            @pl.when(sector % 2 == parity)
            def _():
                body(1 - parity, parity)

    def fix_layer(k, upper, given):
        a = layers - 1 if upper else 0
        for m in range(comps):
            total = axial[upper, plane(m)] * given[0]
            for n in range(1, comps):
                total = total + axial[upper, plane(n * comps + m)] * given[n]
            add_plane(k, a, m, total)

    def fix_upper(k):
        rim_copy(k, 1).wait_recv()
        fix_layer(k, 1, [rim_in[k, 1, n] for n in range(comps)])

    def fix_lower(k):
        rim_copy(k, 0).wait_recv()
        fix_layer(k, 0, [rim_in[k, 0, n] for n in range(comps)])

    def relay(k):
        all_rows(k).wait_recv()
        for step in near_last:
            if step:
                forward[k, step] = rows[k][chosen[step]]
                forward_copy(k, step).start()
            else:
                picked[k][low] = rows[k][chosen[step]]

    def relay_cross():
        all_crosses().wait_recv()
        for step in near_last:
            if step:
                cross_forward[step] = cross[chosen[step]]
                cross_forward_copy(step).start()
            else:
                cross_picked[low] = cross[chosen[step]]

    def got(k, j, n, c):
        return picked[k][slots[j], n, c : c + 1, :]

    def crossing(k):
        def one(j, side, other, c):
            total = None
            for n in range(comps):
                start = side * pairs + n * comps
                term = cross_picked[slots[j], start : start + comps, :] * got(k - 1, other, n, c)
                total = term if total is None else total + term
            return total

        return one(1, 1, 0, around - 1), one(1, 0, 2, 0), one(2, 1, 1, around - 1)

    def facing_of(k, extra):
        values = []
        for n in range(comps):
            total = blend[plane(around)] * got(k, 2, n, 0)
            for c in range(around):
                total = total + blend[plane(c)] * got(k, 1, n, c)
            if extra is not None:
                begin, end, next_begin = extra
                total = total + blend[plane(0)] * begin[n : n + 1] + blend[plane(around - 1)] * end[n : n + 1]
                total = total + blend[plane(around)] * next_begin[n : n + 1]
            values.append(total)
        return values

    def facing_beside(k, s):
        most, last = (0, 1) if s == 0 else (2, 3)
        ratios = near_in[s, pl.ds(mixing, around)]
        ratio = near_in[s, pl.ds(mixing + around, 1)]
        total = None
        for n in range(comps):
            value = jnp.sum(ratios * picked[k][slots[most], n], axis=0, keepdims=True) + ratio * got(k, last, n, 0)
            term = near_in[s, pl.ds(comps + pairs + n * comps, comps)] * value
            total = term if total is None else total + term
        return total

    def complete_parts(k):
        for s in range(2):
            where = pl.ds(0, comps, stride=layers)
            part_in[k // 2, s, where] = part_in[k // 2, s, where] + facing_beside(k, s)

    def complete_near():
        for s in range(2):
            total = near_in[s, pl.ds(0, comps)] + facing_beside(0, s)
            for n in range(comps):
                total = total + near_in[s, pl.ds(comps + n * comps, comps)] * edge[0, 1 - s, pl.ds(n * layers, 1)]
            near_halo[s] = total

    def fix_near():
        for side in range(2):
            total = None
            for n in range(comps):
                term = near[side, pl.ds(comps + n * comps, comps)] * near_halo[1 - side, pl.ds(n, 1)]
                total = term if total is None else total + term
            for m in range(comps):
                where = pl.ds(around + rims[side], 1)
                field[2, m, where] = field[2, m, where] + total[m : m + 1]

    def wait_forward(k):
        all_forwards(k).wait_recv()

    def wait_sends():
        coef_copy(0).wait_send()
        both_edges(0).wait_send()
        both_edges(2).wait_send()
        both_parts(2).wait_send()
        @pl.when(block > 0)
        def _():
            sent_rims(1).wait_send()

        @pl.when(has_upper)
        def _():
            sent_rims(0).wait_send()

        @pl.when(is_rotor_face)
        def _():
            all_crosses().wait_send()
            sent_rows().wait_send()

        @pl.when(is_stator_face)
        def _():
            both_near().wait_send()
            both_edges(1).wait_send()
            all_cross_forwards().wait_send()
            sent_forwards().wait_send()

        @pl.when(~is_stator_face)
        def _():
            edge_copy(1, 0).wait_send()
            part_copy(0, 0).wait_send()

    def arrive(k, side):
        edge_copy(k, 1 - side).wait_recv()

    for k in range(ITERS):
        last = k == ITERS - 1
        even = k % 2 == 0
        make_radial(k)
        local_parts(k, 0, layers)
        if last:
            for m in range(comps):
                update_ref[m] = field[k, m, pl.ds(around, layers * around)]

        @pl.when(has_lower)
        def _():
            fix_lower(k)

        if even:

            @pl.when(block < blocks - 1)
            def _():
                fix_upper(k)

            @pl.when(is_rotor_face)
            def _():
                for n in range(comps):
                    row_out[k // 2, n] = field[k + 1, n, plane(layers)]
                send_rows(k + 1)

            if k == 0:

                @pl.when(is_start)
                def _():
                    pl.semaphore_wait(ready, 1)
                    edge_copy(0, 1).start()

                @pl.when(is_stator_face)
                def _():
                    for side in range(2):
                        for m in range(comps):
                            near[side, pl.ds(m, 1)] = field[1, m, pl.ds(around + rims[side], 1)]
                        near_copy(side).start()

            def begin(far, close):
                if k == 0:

                    @pl.when(~is_stator_face)
                    def _():
                        coef_copy(far).start()
                        send_part(0, far)

                else:
                    send_part(k, far)
                arrive(k, close)
                fix_side(k, close, received)
                if k == 0:
                    take_edges(1, (close,))
                    edge_copy(1, close).start()
                else:
                    send_part(k, close)

                @pl.when(is_stator_face)
                def _():
                    relay(k)

                arrive(k, far)
                fix_side(k, far, received)
                if k == 0:

                    @pl.when(is_stator_face)
                    def _():
                        take_edges(1, (far,))
                        edge_copy(1, far).start()

            by_place(begin)

            @pl.when(is_stator_face)
            def _():
                if k == 0:
                    relay_cross()
                relay(k + 1)
                if k == 0:
                    by_place(lambda far, close: coef_copy(far).start())
                    both_near().wait_recv()
                wait_forward(k)
                fix_layer(k, 0, facing_of(k, None))

            send_rims(k + 1)
        elif not last:

            @pl.when(is_stator_face)
            def _():
                complete_near()
                fix_near()
                all_cross_forwards().wait_recv()
                extra = crossing(k)

                @pl.when(block < blocks - 1)
                def _():
                    fix_upper(k)

                wait_forward(k)
                fix_layer(k, 0, facing_of(k, extra))
                rim_copy(k + 1, 1).start()
                for side in range(2):
                    arrive(1, side)
                    fix_side(k, side, received, 1)

            @pl.when(~is_stator_face)
            def _():
                def finish(far, close):
                    arrive(1, close)
                    fix_side(k, close, received)
                    part_copy(0, 1 - far).wait_recv()
                    coef_copy(1 - far).wait_recv()
                    fix_side(k, far, completed)

                by_place(finish)

                @pl.when(block < blocks - 1)
                def _():
                    fix_upper(k)

                @pl.when(is_rotor_face)
                def _():
                    send_rows(k + 1)

                @pl.when(block > 0)
                def _():
                    rim_copy(k + 1, 1).start()

            @pl.when(has_upper)
            def _():
                rim_copy(k + 1, 0).start()

            take_edges(k + 1)

            def exchange(far, close):
                edge_copy(k + 1, far).start()
                edge_copy(k + 1, close).start()

            by_place(exchange)
        else:
            both_parts(2).wait_recv()

            @pl.when(is_stator_face)
            def _():
                coef_copy(0).wait_recv()
                complete_parts(2)

            def end(far, close):
                fix_side(k, close, sent)
                fix_side(k, far, completed)

            by_place(end)
            wait_sends()

            @pl.when(block < blocks - 1)
            def _():
                fix_upper(k)

            @pl.when(is_stator_face)
            def _():
                extra = crossing(k)
                wait_forward(k)
                fix_layer(k, 0, facing_of(k, extra))


UNROLL = 2


def solution(mesh):
    sectors, blocks = mesh.shape["sector"], mesh.shape["block"]
    lows = low_part(sectors)
    highs = sectors // lows

    def sweeps(prev, source, face, inverse, offset, cells, weights):
        comps, layers, around, lanes = prev.shape
        f32, dma = jnp.float32, pltpu.SemaphoreType.DMA
        flat = (comps, layers * around, lanes)
        pairs = comps * comps
        row = (comps, around, lanes)
        cross = (2 * pairs, lanes)
        sides = (2, comps * layers, lanes)
        near = (2, comps + 2 * pairs + around + 1, lanes)
        hbm = pl.BlockSpec(memory_space=pl.ANY)
        vmem = pl.BlockSpec(memory_space=pltpu.VMEM)
        negative, previous = pl.pallas_call(
            functools.partial(kernel, sectors, blocks, layers, around),
            out_shape=(pltpu.VMEM(flat, f32),) * 2,
            in_specs=[hbm] * 7,
            out_specs=(vmem, vmem),
            scratch_shapes=[
                pltpu.SMEM(offset.shape, offset.dtype),
                pltpu.SMEM(cells.shape, cells.dtype),
                pltpu.SMEM(weights.shape, weights.dtype),
                pltpu.VMEM((ITERS, comps, (layers + 2) * around, lanes), f32),
                pltpu.VMEM(flat, f32),
                pltpu.VMEM(face.shape, face.dtype),
                pltpu.VMEM(inverse.shape, inverse.dtype),
                pltpu.VMEM((3, comps) + flat, f32),
                pltpu.VMEM((comps,) + flat, f32),
                pltpu.VMEM(flat, f32),
                pltpu.VMEM((3,) + sides, f32),
                pltpu.VMEM((3,) + sides, f32),
                pltpu.VMEM((2,) + sides, f32),
                pltpu.VMEM((2,) + sides, f32),
                pltpu.VMEM((2, pairs * layers, lanes), f32),
                pltpu.VMEM((2, pairs * layers, lanes), f32),
                pltpu.VMEM(near, f32),
                pltpu.VMEM(near, f32),
                pltpu.VMEM((2, comps, lanes), f32),
                pltpu.VMEM((2, pairs * around, lanes), f32),
                pltpu.VMEM((ITERS, 2) + row, f32),
                pltpu.VMEM((2,) + row, f32),
                [pltpu.VMEM((highs,) + row, f32)] * ITERS,
                pltpu.VMEM((ITERS, lows) + row, f32),
                [pltpu.VMEM((lows,) + row, f32)] * ITERS,
                pltpu.VMEM(cross, f32),
                pltpu.VMEM((highs,) + cross, f32),
                pltpu.VMEM((lows,) + cross, f32),
                pltpu.VMEM((lows,) + cross, f32),
                pltpu.VMEM(((around + 1) * around, lanes), f32),
                dma((7,)),
                pltpu.SemaphoreType.REGULAR,
                dma((3,)),
                dma((3, 2)),
                dma((2,)),
                dma((2,)),
                dma,
                dma,
                dma,
                dma,
                dma((min(blocks - 1, 2),)),
                dma((ITERS, min(blocks - 1, 2))),
                dma,
                dma((ITERS,)),
                dma,
                dma((ITERS,)),
                dma,
                dma,
                dma,
                dma,
            ],
            compiler_params=pltpu.CompilerParams(collective_id=0, has_side_effects=True),
        )(prev.reshape(flat), source.reshape(flat), face, inverse, offset, cells, weights)
        negative, previous = negative.reshape(prev.shape), previous.reshape(prev.shape)
        return 0.0 - negative, 0.0 - negative - previous

    return jax.shard_map(
        sweeps,
        mesh=mesh,
        in_specs=(
            P(None, "block", "sector", None),
            P(None, "block", "sector", None),
            P(None, None, None, "block", "sector", None),
            P(None, None, "block", "sector", None),
            P(),
            P("sector"),
            P("sector"),
        ),
        out_specs=(P(None, "block", "sector", None), P(None, "block", "sector", None)),
        check_vma=False,
    )
```

```python
import functools

import jax
import jax.numpy as jnp
from jax import lax
from jax.experimental import pallas as pl
from jax.experimental.pallas import tpu as pltpu
from jax.sharding import PartitionSpec as P

ITERS = 4
LOWER, UPPER = 0.6, 0.4
MESH = pl.DeviceIdType.MESH


def low_part(sectors):
    return min(d for d in range(1, sectors + 1) if sectors % d == 0 and d * d >= sectors)


def kernel(
    sectors,
    blocks,
    layers,
    around,
    prev_ref,
    source_ref,
    face_ref,
    inverse_ref,
    offset_hbm,
    cells_hbm,
    weights_hbm,
    adjoint_ref,
    update_ref,
    offset_ref,
    cells_ref,
    weights_ref,
    field,
    source,
    face16,
    inverse16,
    face,
    inverse,
    radial,
    edge,
    halo,
    part,
    part_in,
    coef,
    coef_in,
    near,
    near_in,
    near_halo,
    axial,
    rim_in,
    row_out,
    rows,
    forward,
    picked,
    cross_out,
    cross,
    cross_forward,
    cross_picked,
    blend,
    local_sem,
    ready,
    edge_send,
    edge_recv,
    part_send,
    part_recv,
    coef_send,
    coef_recv,
    near_send,
    near_recv,
    rim_send,
    rim_recv,
    row_send,
    row_recv,
    forward_send,
    forward_recv,
    cross_send,
    cross_recv,
    cross_forward_send,
    cross_forward_recv,
):
    comps, _, lanes = prev_ref.shape
    pairs = comps * comps
    mixing = comps + 2 * pairs
    sector = lax.axis_index("sector")
    block = lax.axis_index("block")
    first = blocks // 2
    lows = low_part(sectors)
    highs = sectors // lows
    high, low = sector // lows, sector % lows
    after, before = (sector + 1) % sectors, (sector + sectors - 1) % sectors
    is_stator_face = block == first
    is_rotor_face = block == first - 1
    has_lower = (block > 0) & (block != first)
    has_upper = (block < blocks - 1) & (block != first - 1)
    rims = (around - 1, 0)

    def partner(step):
        return low ^ step if lows & (lows - 1) == 0 else (low + step) % lows

    barrier = pltpu.get_barrier_semaphore()

    def greet(to_sector, to_block):
        pl.semaphore_signal(barrier, inc=1, device_id=(to_sector, to_block), device_id_type=MESH)

    is_end = sector == sectors - 1
    is_start = sector == 0

    @pl.when(~is_end)
    def _():
        greet(after, block)

    greet(before, block)

    @pl.when(block > 0)
    def _():
        greet(sector, block - 1)

    @pl.when(block < blocks - 1)
    def _():
        greet(sector, block + 1)

    @pl.when(is_stator_face)
    def _():
        for step in range(highs):
            greet(((high + step) % highs) * lows + low, first - 1)
        for step in range(1, lows):
            greet(high * lows + partner(step), first)

    def plane(a):
        return pl.ds(a * around, around) if isinstance(a, int) else pl.ds(pl.multiple_of(a * around, around), around)

    def column_of(c, start=0):
        return pl.ds(start + c, layers, stride=around)

    def item(n):
        return pl.ds(n * layers, layers)

    into_field = pltpu.make_async_copy(prev_ref, field.at[0, :, pl.ds(around, layers * around)], local_sem.at[0])
    into_source = pltpu.make_async_copy(source_ref, source, local_sem.at[1])
    into_face = pltpu.make_async_copy(face_ref, face16, local_sem.at[2])
    into_inverse = pltpu.make_async_copy(inverse_ref, inverse16, local_sem.at[3])
    into_offset = pltpu.make_async_copy(offset_hbm, offset_ref, local_sem.at[4])
    into_cells = pltpu.make_async_copy(cells_hbm, cells_ref, local_sem.at[5])
    into_weights = pltpu.make_async_copy(weights_hbm, weights_ref, local_sem.at[6])
    scalars = (into_offset, into_cells, into_weights)
    for copy in (into_field,) + scalars + (into_inverse, into_face, into_source):
        copy.start()

    greetings = 2 - is_start.astype(jnp.int32) + (block > 0).astype(jnp.int32) + (block < blocks - 1).astype(jnp.int32)
    greetings += jnp.where(is_rotor_face, highs, 0) + jnp.where(is_stator_face, lows - 1, 0)

    @pl.when(is_end)
    def _():
        pl.semaphore_wait(barrier, greetings)
        pl.semaphore_signal(ready, inc=1, device_id=(after, block), device_id_type=MESH)

    nothing = jnp.zeros((around, lanes), jnp.float32)
    for k in range(ITERS):
        for n in range(comps):
            field[k, n, plane(0)] = nothing
            field[k, n, plane(layers + 1)] = nothing

    for copy in scalars:
        copy.wait()
    column = lax.broadcasted_iota(jnp.int32, (around, lanes), 0)
    lane = lax.broadcasted_iota(jnp.int32, (around, lanes), 1)
    donor = jnp.zeros((around, lanes), jnp.int32)
    weight = jnp.zeros((around, lanes), jnp.float32)
    for j in range(around):
        donor = jnp.where(column == j, cells_ref[j], donor)
        weight = jnp.where(column == j, weights_ref[j], weight)
    for c in range(around + 1):
        blend[plane(c)] = jnp.where(donor == c, weight, 0.0) + jnp.where(donor + 1 == c, 1.0 - weight, 0.0)
    radial_lower = jnp.where(lane == 0, 0.0, LOWER).astype(jnp.float32)
    radial_upper = jnp.where(lane == lanes - 1, 0.0, UPPER).astype(jnp.float32)
    around_lower = jnp.where(column == 0, 0.0, LOWER).astype(jnp.float32)
    around_upper = jnp.where(column == around - 1, 0.0, UPPER).astype(jnp.float32)

    offset = offset_ref[0]
    chosen = []
    for step in range(lows):
        to = high * lows + partner(step)
        base = to + 2 * sectors - offset - 1
        ahead = lax.rem(low + lows - lax.rem(base, lows), lows)
        chosen.append(lax.rem(lax.div(base + ahead, lows), highs))
    slots = [lax.rem(low + 2 * sectors - offset - 1 + j, lows) for j in range(4)]

    into_field.wait()

    def slot_of(k):
        return (0, 2, 1)[k]

    def take_edges(k, sides=(0, 1)):
        for side in sides:
            for n in range(comps):
                edge[slot_of(k), side, item(n)] = field[k, n, column_of(rims[side], around)]

    take_edges(0)

    def remote(src, dst, send, recv, to):
        return pltpu.make_async_remote_copy(
            src_ref=src, dst_ref=dst, send_sem=send, recv_sem=recv, device_id=to, device_id_type=MESH
        )

    def beside(side):
        return (before if side else after, block)

    def edge_copy(k, side):
        i = slot_of(k)
        return remote(edge.at[i, side], halo.at[i, side], edge_send.at[i], edge_recv.at[i, side], beside(side))

    def part_copy(k, side):
        i = k // 2
        return remote(part.at[i, side], part_in.at[i, side], part_send.at[i], part_recv.at[i], beside(side))

    def coef_copy(side):
        return remote(coef.at[side], coef_in.at[side], coef_send, coef_recv, beside(side))

    def coef_pieces(side, pieces):
        for n in pieces:
            piece = pl.ds(n * comps * layers, comps * layers)
            remote(coef.at[side, piece], coef_in.at[side, piece], coef_send, coef_recv, beside(side)).start()

    def near_copy(side):
        return remote(near.at[side], near_in.at[side], near_send, near_recv, beside(side))

    def rim_copy(k, side):
        return remote(
            field.at[k, :, plane(1 if side else layers)],
            rim_in.at[k, side],
            rim_send.at[1 - side],
            rim_recv.at[k, 1 - side],
            (sector, block - 1 if side else block + 1),
        )

    def sent_rims(side):
        ours = rim_in.at[:, side]
        to = (sector, block - 1 if side else block + 1)
        return remote(ours, ours, rim_send.at[1 - side], rim_recv.at[0, 1 - side], to)

    def row_source(k):
        return row_out.at[k // 2] if k % 2 else field.at[k, :, plane(layers)]

    def row_copy(k, step):
        to = (high + step) % highs
        return remote(row_source(k), rows[k].at[high], row_send, row_recv.at[k], (to * lows + low, first))

    def all_rows(k):
        return remote(rows[k], rows[k], row_send, row_recv.at[k], (sector, first))

    def sent_rows():
        part = forward.at[:, pl.ds(0, highs)]
        return remote(part, part, row_send, row_recv.at[0], (sector, first))

    def cross_copy(step):
        to = (high + step) % highs
        return remote(cross_out, cross.at[high], cross_send, cross_recv, (to * lows + low, first))

    def all_crosses():
        return remote(cross, cross, cross_send, cross_recv, (sector, first))

    def forward_copy(k, step):
        to = (high * lows + partner(step), first)
        return remote(forward.at[k, step], picked[k].at[low], forward_send, forward_recv.at[k], to)

    def all_forwards(k):
        part = forward.at[k, pl.ds(1, lows - 1)]
        return remote(part, part, forward_send, forward_recv.at[k], (sector, first))

    def sent_forwards():
        part = forward.at[:, pl.ds(1, lows - 1)]
        return remote(part, part, forward_send, forward_recv.at[0], (sector, first))

    def cross_forward_copy(step):
        to = (high * lows + partner(step), first)
        return remote(
            cross_forward.at[step], cross_picked.at[low], cross_forward_send, cross_forward_recv, to
        )

    def all_cross_forwards():
        part = cross_forward.at[pl.ds(1, lows - 1)]
        return remote(part, part, cross_forward_send, cross_forward_recv, (sector, first))

    def both_edges(k):
        i = slot_of(k)
        return remote(edge.at[i], halo.at[i], edge_send.at[i], edge_recv.at[i, 0], beside(0))

    def both_parts(k):
        i = k // 2
        return remote(part.at[i], part_in.at[i], part_send.at[i], part_recv.at[i], beside(0))

    def both_near():
        return remote(near, near_in, near_send, near_recv, beside(0))

    near_last = sorted(range(lows), key=lambda step: -bin(step).count("1"))
    far_first = sorted(range(highs), key=lambda step: -min(step, highs - step))

    def send_rows(k):
        for step in far_first:
            row_copy(k, step).start()

    def send_rims(k):
        @pl.when(block > 0)
        def _():
            rim_copy(k, 1).start()

        @pl.when(has_upper)
        def _():
            rim_copy(k, 0).start()

    @pl.when(~is_end)
    def _():
        pl.semaphore_wait(barrier, greetings)

    send_rims(0)

    @pl.when(is_rotor_face)
    def _():
        send_rows(0)

    edge_copy(0, 0).start()

    @pl.when(~is_start)
    def _():
        edge_copy(0, 1).start()

    into_inverse.wait()

    def widen_inverse(i, carry):
        for m in range(comps):
            inverse[i, m] = inverse16[i, m].astype(jnp.float32).reshape(layers * around, lanes)
        return carry

    lax.fori_loop(0, comps, widen_inverse, 0)
    into_face.wait()

    def widen(i, carry):
        for d in range(3):
            for m in range(comps):
                face[d, i, m] = face16[d, i, m].astype(jnp.float32).reshape(layers * around, lanes)
        return carry

    lax.fori_loop(0, comps, widen, 0)

    def product(direction, where, share, store):
        inv = [[inverse[p, m, where] for m in range(comps)] for p in range(comps)]

        def body(n, carry):
            give = [share * face[direction, n, m, where] for m in range(comps)]
            for p in range(comps):
                total = inv[p][0] * give[0]
                for m in range(1, comps):
                    total = total + inv[p][m] * give[m]
                store(n * comps + p, total)
            return carry

        lax.fori_loop(0, comps, body, 0)

    for side in range(2):

        def keep(i, value):
            coef[side, pl.ds(pl.multiple_of(i * layers, layers), layers)] = value

        product(1, column_of(rims[side]), LOWER if side else UPPER, keep)

    @pl.when(is_rotor_face)
    def _():
        for side in range(2):
            for n in range(comps):
                cross_out[pl.ds(side * pairs + n * comps, comps)] = coef[
                    side, pl.ds(n * comps * layers + layers - 1, comps, stride=layers)
                ]
        for step in far_first:
            cross_copy(step).start()

    for side, (a, share) in enumerate(((0, LOWER), (layers - 1, UPPER))):

        def keep(i, value):
            axial[side, pl.ds(pl.multiple_of(i * around, around), around)] = value

        product(0, plane(a), share, keep)

    @pl.when(is_stator_face)
    def _():
        for side in range(2):
            for n in range(comps):
                near[side, pl.ds(comps + n * comps, comps)] = coef[side, pl.ds(n * comps * layers, comps, stride=layers)]
                near[side, pl.ds(comps + pairs + n * comps, comps)] = axial[
                    0, pl.ds(n * comps * around + rims[side], comps, stride=around)
                ]
            near[side, pl.ds(mixing, around)] = blend[pl.ds(rims[side], around, stride=around)]
            near[side, pl.ds(mixing + around, 1)] = blend[pl.ds(around * around + rims[side], 1)]

    into_source.wait()

    def make_radial(k):
        for n in range(comps):
            for a in range(layers):
                here = field[k, n, plane(a + 1)]
                radial[n, plane(a)] = radial_lower * pltpu.roll(here, 1, 1) + radial_upper * pltpu.roll(here, lanes - 1, 1)

    def local_part(k, a):
        acc = [source[m, plane(a)] for m in range(comps)]
        for n in range(comps):
            mix = radial[n, plane(a)]
            acc = [acc[m] + face[2, n, m, plane(a)] * mix for m in range(comps)]
        for n in range(comps):
            here = field[k, n, plane(a + 1)]
            mix = around_lower * pltpu.roll(here, 1, 0) + around_upper * pltpu.roll(here, around - 1, 0)
            acc = [acc[m] + face[1, n, m, plane(a)] * mix for m in range(comps)]
        for n in range(comps):
            mix = LOWER * field[k, n, plane(a)] + UPPER * field[k, n, plane(a + 2)]
            acc = [acc[m] + face[0, n, m, plane(a)] * mix for m in range(comps)]
        for m in range(comps):
            fresh = inverse[m, 0, plane(a)] * acc[0]
            for n in range(1, comps):
                fresh = fresh + inverse[m, n, plane(a)] * acc[n]
            if k < ITERS - 1:
                field[k + 1, m, plane(a + 1)] = fresh
            else:
                adjoint_ref[m, plane(a)] = 0.0 - fresh

    def send_part(k, side):
        for n in range(comps):
            part[k // 2, side, item(n)] = field[k + 1, n, column_of(rims[side], around)]
        part_copy(k, side).start()

    def local_parts(k, start, stop):
        def body(a, carry):
            local_part(k, a)
            return carry

        lax.fori_loop(start, stop, body, 0, unroll=UNROLL)

    def add_column(k, side, m, value, skip=0):
        if k < ITERS - 1:
            where = pl.ds((1 + skip) * around + rims[side], layers - skip, stride=around)
            value = value[skip:]
            field[k + 1, m, where] = field[k + 1, m, where] + value
        else:
            where = column_of(rims[side])
            adjoint_ref[m, where] = adjoint_ref[m, where] - value

    def add_plane(k, a, m, value):
        if k < ITERS - 1:
            field[k + 1, m, plane(a + 1)] = field[k + 1, m, plane(a + 1)] + value
        else:
            adjoint_ref[m, plane(a)] = adjoint_ref[m, plane(a)] - value

    def completed(k, s):
        i = k // 2
        own = [edge[i, 1 - s, item(n)] for n in range(comps)]
        values = []
        for m in range(comps):
            total = part_in[i, s, item(m)]
            for n in range(comps):
                total = total + coef_in[s, item(n * comps + m)] * own[n]
            values.append(total)
        return values

    def sent(k, s):
        return [part_in[k // 2, s, item(n)] for n in range(comps)]

    def received(k, s):
        return [halo[slot_of(k), s, item(n)] for n in range(comps)]

    def fix_side(k, side, halo_of, skip=0):
        given = halo_of(k, 1 - side)
        for m in range(comps):
            total = coef[side, item(m)] * given[0]
            for n in range(1, comps):
                total = total + coef[side, item(n * comps + m)] * given[n]
            add_column(k, side, m, total, skip)

    def by_place(body):
        for parity in range(2):

            @pl.when(sector % 2 == parity)
            def _():
                body(1 - parity, parity)

    def fix_layer(k, upper, given):
        a = layers - 1 if upper else 0
        for m in range(comps):
            total = axial[upper, plane(m)] * given[0]
            for n in range(1, comps):
                total = total + axial[upper, plane(n * comps + m)] * given[n]
            add_plane(k, a, m, total)

    def fix_upper(k):
        rim_copy(k, 1).wait_recv()
        fix_layer(k, 1, [rim_in[k, 1, n] for n in range(comps)])

    def fix_lower(k):
        rim_copy(k, 0).wait_recv()
        fix_layer(k, 0, [rim_in[k, 0, n] for n in range(comps)])

    def relay(k):
        all_rows(k).wait_recv()
        for step in near_last:
            if step:
                forward[k, step] = rows[k][chosen[step]]
                forward_copy(k, step).start()
            else:
                picked[k][low] = rows[k][chosen[step]]

    def relay_cross():
        all_crosses().wait_recv()
        for step in near_last:
            if step:
                cross_forward[step] = cross[chosen[step]]
                cross_forward_copy(step).start()
            else:
                cross_picked[low] = cross[chosen[step]]

    def got(k, j, n, c):
        return picked[k][slots[j], n, c : c + 1, :]

    def crossing(k):
        def one(j, side, other, c):
            total = None
            for n in range(comps):
                start = side * pairs + n * comps
                term = cross_picked[slots[j], start : start + comps, :] * got(k - 1, other, n, c)
                total = term if total is None else total + term
            return total

        return one(1, 1, 0, around - 1), one(1, 0, 2, 0), one(2, 1, 1, around - 1)

    def facing_of(k, extra):
        values = []
        for n in range(comps):
            total = blend[plane(around)] * got(k, 2, n, 0)
            for c in range(around):
                total = total + blend[plane(c)] * got(k, 1, n, c)
            if extra is not None:
                begin, end, next_begin = extra
                total = total + blend[plane(0)] * begin[n : n + 1] + blend[plane(around - 1)] * end[n : n + 1]
                total = total + blend[plane(around)] * next_begin[n : n + 1]
            values.append(total)
        return values

    def facing_beside(k, s):
        most, last = (0, 1) if s == 0 else (2, 3)
        ratios = near_in[s, pl.ds(mixing, around)]
        ratio = near_in[s, pl.ds(mixing + around, 1)]
        total = None
        for n in range(comps):
            value = jnp.sum(ratios * picked[k][slots[most], n], axis=0, keepdims=True) + ratio * got(k, last, n, 0)
            term = near_in[s, pl.ds(comps + pairs + n * comps, comps)] * value
            total = term if total is None else total + term
        return total

    def complete_parts(k):
        for s in range(2):
            where = pl.ds(0, comps, stride=layers)
            part_in[k // 2, s, where] = part_in[k // 2, s, where] + facing_beside(k, s)

    def complete_near():
        for s in range(2):
            total = near_in[s, pl.ds(0, comps)] + facing_beside(0, s)
            for n in range(comps):
                total = total + near_in[s, pl.ds(comps + n * comps, comps)] * edge[0, 1 - s, pl.ds(n * layers, 1)]
            near_halo[s] = total

    def fix_near():
        for side in range(2):
            total = None
            for n in range(comps):
                term = near[side, pl.ds(comps + n * comps, comps)] * near_halo[1 - side, pl.ds(n, 1)]
                total = term if total is None else total + term
            for m in range(comps):
                where = pl.ds(around + rims[side], 1)
                field[2, m, where] = field[2, m, where] + total[m : m + 1]

    def wait_forward(k):
        all_forwards(k).wait_recv()

    def wait_sends():
        coef_copy(0).wait_send()
        both_edges(0).wait_send()
        both_edges(2).wait_send()
        both_parts(2).wait_send()
        @pl.when(block > 0)
        def _():
            sent_rims(1).wait_send()

        @pl.when(has_upper)
        def _():
            sent_rims(0).wait_send()

        @pl.when(is_rotor_face)
        def _():
            all_crosses().wait_send()
            sent_rows().wait_send()

        @pl.when(is_stator_face)
        def _():
            both_near().wait_send()
            both_edges(1).wait_send()
            all_cross_forwards().wait_send()
            sent_forwards().wait_send()

        @pl.when(~is_stator_face)
        def _():
            edge_copy(1, 0).wait_send()
            part_copy(0, 0).wait_send()

    def arrive(k, side):
        edge_copy(k, 1 - side).wait_recv()

    for k in range(ITERS):
        last = k == ITERS - 1
        even = k % 2 == 0
        make_radial(k)
        local_parts(k, 0, layers)
        if last:
            for m in range(comps):
                update_ref[m] = field[k, m, pl.ds(around, layers * around)]

        @pl.when(has_lower)
        def _():
            fix_lower(k)

        if even:

            @pl.when(block < blocks - 1)
            def _():
                fix_upper(k)

            @pl.when(is_rotor_face)
            def _():
                for n in range(comps):
                    row_out[k // 2, n] = field[k + 1, n, plane(layers)]
                send_rows(k + 1)

            if k == 0:

                @pl.when(is_start)
                def _():
                    pl.semaphore_wait(ready, 1)
                    edge_copy(0, 1).start()

                @pl.when(is_stator_face)
                def _():
                    for side in range(2):
                        for m in range(comps):
                            near[side, pl.ds(m, 1)] = field[1, m, pl.ds(around + rims[side], 1)]
                        near_copy(side).start()

            def begin(far, close):
                if k == 0:

                    @pl.when(~is_stator_face)
                    def _():
                        coef_pieces(far, range(comps))
                        send_part(0, far)

                else:
                    send_part(k, far)
                arrive(k, close)
                fix_side(k, close, received)
                if k == 0:
                    take_edges(1, (close,))
                    edge_copy(1, close).start()
                else:
                    send_part(k, close)

                @pl.when(is_stator_face)
                def _():
                    relay(k)

                arrive(k, far)
                fix_side(k, far, received)
                if k == 0:

                    @pl.when(is_stator_face)
                    def _():
                        take_edges(1, (far,))
                        edge_copy(1, far).start()

            by_place(begin)

            @pl.when(is_stator_face)
            def _():
                if k == 0:
                    relay_cross()
                relay(k + 1)
                if k == 0:
                    by_place(lambda far, close: coef_pieces(far, range(0, 2)))
                    both_near().wait_recv()
                wait_forward(k)
                fix_layer(k, 0, facing_of(k, None))
                if k == 0:
                    by_place(lambda far, close: coef_pieces(far, range(2, 4)))

            send_rims(k + 1)
        elif not last:

            @pl.when(is_stator_face)
            def _():
                complete_near()
                fix_near()
                all_cross_forwards().wait_recv()
                extra = crossing(k)

                @pl.when(block < blocks - 1)
                def _():
                    fix_upper(k)

                wait_forward(k)
                fix_layer(k, 0, facing_of(k, extra))
                rim_copy(k + 1, 1).start()
                for side in range(2):
                    arrive(1, side)
                    fix_side(k, side, received, 1)

            @pl.when(~is_stator_face)
            def _():
                def finish(far, close):
                    arrive(1, close)
                    fix_side(k, close, received)
                    part_copy(0, 1 - far).wait_recv()
                    coef_copy(1 - far).wait_recv()
                    fix_side(k, far, completed)

                by_place(finish)

                @pl.when(block < blocks - 1)
                def _():
                    fix_upper(k)

                @pl.when(is_rotor_face)
                def _():
                    send_rows(k + 1)

                @pl.when(block > 0)
                def _():
                    rim_copy(k + 1, 1).start()

            @pl.when(has_upper)
            def _():
                rim_copy(k + 1, 0).start()

            take_edges(k + 1)

            def exchange(far, close):
                edge_copy(k + 1, far).start()
                edge_copy(k + 1, close).start()

                @pl.when(is_stator_face)
                def _():
                    coef_pieces(far, range(4, comps))

            by_place(exchange)
        else:
            both_parts(2).wait_recv()

            @pl.when(is_stator_face)
            def _():
                coef_copy(0).wait_recv()
                complete_parts(2)

            def end(far, close):
                fix_side(k, close, sent)
                fix_side(k, far, completed)

            by_place(end)
            wait_sends()

            @pl.when(block < blocks - 1)
            def _():
                fix_upper(k)

            @pl.when(is_stator_face)
            def _():
                extra = crossing(k)
                wait_forward(k)
                fix_layer(k, 0, facing_of(k, extra))


UNROLL = 2


def solution(mesh):
    sectors, blocks = mesh.shape["sector"], mesh.shape["block"]
    lows = low_part(sectors)
    highs = sectors // lows

    def sweeps(prev, source, face, inverse, offset, cells, weights):
        comps, layers, around, lanes = prev.shape
        f32, dma = jnp.float32, pltpu.SemaphoreType.DMA
        flat = (comps, layers * around, lanes)
        pairs = comps * comps
        row = (comps, around, lanes)
        cross = (2 * pairs, lanes)
        sides = (2, comps * layers, lanes)
        near = (2, comps + 2 * pairs + around + 1, lanes)
        hbm = pl.BlockSpec(memory_space=pl.ANY)
        vmem = pl.BlockSpec(memory_space=pltpu.VMEM)
        negative, previous = pl.pallas_call(
            functools.partial(kernel, sectors, blocks, layers, around),
            out_shape=(pltpu.VMEM(flat, f32),) * 2,
            in_specs=[hbm] * 7,
            out_specs=(vmem, vmem),
            scratch_shapes=[
                pltpu.SMEM(offset.shape, offset.dtype),
                pltpu.SMEM(cells.shape, cells.dtype),
                pltpu.SMEM(weights.shape, weights.dtype),
                pltpu.VMEM((ITERS, comps, (layers + 2) * around, lanes), f32),
                pltpu.VMEM(flat, f32),
                pltpu.VMEM(face.shape, face.dtype),
                pltpu.VMEM(inverse.shape, inverse.dtype),
                pltpu.VMEM((3, comps) + flat, f32),
                pltpu.VMEM((comps,) + flat, f32),
                pltpu.VMEM(flat, f32),
                pltpu.VMEM((3,) + sides, f32),
                pltpu.VMEM((3,) + sides, f32),
                pltpu.VMEM((2,) + sides, f32),
                pltpu.VMEM((2,) + sides, f32),
                pltpu.VMEM((2, pairs * layers, lanes), f32),
                pltpu.VMEM((2, pairs * layers, lanes), f32),
                pltpu.VMEM(near, f32),
                pltpu.VMEM(near, f32),
                pltpu.VMEM((2, comps, lanes), f32),
                pltpu.VMEM((2, pairs * around, lanes), f32),
                pltpu.VMEM((ITERS, 2) + row, f32),
                pltpu.VMEM((2,) + row, f32),
                [pltpu.VMEM((highs,) + row, f32)] * ITERS,
                pltpu.VMEM((ITERS, lows) + row, f32),
                [pltpu.VMEM((lows,) + row, f32)] * ITERS,
                pltpu.VMEM(cross, f32),
                pltpu.VMEM((highs,) + cross, f32),
                pltpu.VMEM((lows,) + cross, f32),
                pltpu.VMEM((lows,) + cross, f32),
                pltpu.VMEM(((around + 1) * around, lanes), f32),
                dma((7,)),
                pltpu.SemaphoreType.REGULAR,
                dma((3,)),
                dma((3, 2)),
                dma((2,)),
                dma((2,)),
                dma,
                dma,
                dma,
                dma,
                dma((min(blocks - 1, 2),)),
                dma((ITERS, min(blocks - 1, 2))),
                dma,
                dma((ITERS,)),
                dma,
                dma((ITERS,)),
                dma,
                dma,
                dma,
                dma,
            ],
            compiler_params=pltpu.CompilerParams(collective_id=0, has_side_effects=True),
        )(prev.reshape(flat), source.reshape(flat), face, inverse, offset, cells, weights)
        negative, previous = negative.reshape(prev.shape), previous.reshape(prev.shape)
        return 0.0 - negative, 0.0 - negative - previous

    return jax.shard_map(
        sweeps,
        mesh=mesh,
        in_specs=(
            P(None, "block", "sector", None),
            P(None, "block", "sector", None),
            P(None, None, None, "block", "sector", None),
            P(None, None, "block", "sector", None),
            P(),
            P("sector"),
            P("sector"),
        ),
        out_specs=(P(None, "block", "sector", None), P(None, "block", "sector", None)),
        check_vma=False,
    )
```

```python
import functools

import jax
import jax.numpy as jnp
from jax import lax
from jax.experimental import pallas as pl
from jax.experimental.pallas import tpu as pltpu
from jax.sharding import PartitionSpec as P

ITERS = 4
LOWER, UPPER = 0.6, 0.4
MESH = pl.DeviceIdType.MESH


def low_part(sectors):
    return min(d for d in range(1, sectors + 1) if sectors % d == 0 and d * d >= sectors)


def kernel(
    sectors,
    blocks,
    layers,
    around,
    prev_ref,
    source_ref,
    face_ref,
    inverse_ref,
    offset_hbm,
    cells_hbm,
    weights_hbm,
    adjoint_ref,
    update_ref,
    offset_ref,
    cells_ref,
    weights_ref,
    field,
    source,
    face16,
    inverse16,
    face,
    inverse,
    radial,
    edge,
    halo,
    part,
    part_in,
    coef,
    coef_in,
    near,
    near_in,
    near_halo,
    axial,
    rim_in,
    row_out,
    rows,
    forward,
    picked,
    cross_out,
    cross,
    cross_forward,
    cross_picked,
    blend,
    local_sem,
    ready,
    edge_send,
    edge_recv,
    part_send,
    part_recv,
    coef_send,
    coef_recv,
    near_send,
    near_recv,
    rim_send,
    rim_recv,
    row_send,
    row_recv,
    forward_send,
    forward_recv,
    cross_send,
    cross_recv,
    cross_forward_send,
    cross_forward_recv,
):
    comps, _, lanes = prev_ref.shape
    pairs = comps * comps
    mixing = comps + 2 * pairs
    sector = lax.axis_index("sector")
    block = lax.axis_index("block")
    first = blocks // 2
    lows = low_part(sectors)
    highs = sectors // lows
    high, low = sector // lows, sector % lows
    after, before = (sector + 1) % sectors, (sector + sectors - 1) % sectors
    is_stator_face = block == first
    is_rotor_face = block == first - 1
    has_lower = (block > 0) & (block != first)
    has_upper = (block < blocks - 1) & (block != first - 1)
    rims = (around - 1, 0)

    def partner(step):
        return low ^ step if lows & (lows - 1) == 0 else (low + step) % lows

    barrier = pltpu.get_barrier_semaphore()

    def greet(to_sector, to_block):
        pl.semaphore_signal(barrier, inc=1, device_id=(to_sector, to_block), device_id_type=MESH)

    is_end = sector == sectors - 1
    is_start = sector == 0

    @pl.when(~is_end)
    def _():
        greet(after, block)

    greet(before, block)

    @pl.when(block > 0)
    def _():
        greet(sector, block - 1)

    @pl.when(block < blocks - 1)
    def _():
        greet(sector, block + 1)

    @pl.when(is_stator_face)
    def _():
        for step in range(highs):
            greet(((high + step) % highs) * lows + low, first - 1)
        for step in range(1, lows):
            greet(high * lows + partner(step), first)

    def plane(a):
        return pl.ds(a * around, around) if isinstance(a, int) else pl.ds(pl.multiple_of(a * around, around), around)

    def column_of(c, start=0):
        return pl.ds(start + c, layers, stride=around)

    def item(n):
        return pl.ds(n * layers, layers)

    into_field = pltpu.make_async_copy(prev_ref, field.at[0, :, pl.ds(around, layers * around)], local_sem.at[0])
    into_source = pltpu.make_async_copy(source_ref, source, local_sem.at[1])
    into_face = pltpu.make_async_copy(face_ref, face16, local_sem.at[2])
    into_inverse = pltpu.make_async_copy(inverse_ref, inverse16, local_sem.at[3])
    into_offset = pltpu.make_async_copy(offset_hbm, offset_ref, local_sem.at[4])
    into_cells = pltpu.make_async_copy(cells_hbm, cells_ref, local_sem.at[5])
    into_weights = pltpu.make_async_copy(weights_hbm, weights_ref, local_sem.at[6])
    scalars = (into_offset, into_cells, into_weights)
    for copy in (into_field,) + scalars + (into_inverse, into_face, into_source):
        copy.start()

    greetings = 2 - is_start.astype(jnp.int32) + (block > 0).astype(jnp.int32) + (block < blocks - 1).astype(jnp.int32)
    greetings += jnp.where(is_rotor_face, highs, 0) + jnp.where(is_stator_face, lows - 1, 0)

    @pl.when(is_end)
    def _():
        pl.semaphore_wait(barrier, greetings)
        pl.semaphore_signal(ready, inc=1, device_id=(after, block), device_id_type=MESH)

    nothing = jnp.zeros((around, lanes), jnp.float32)
    for k in range(ITERS):
        for n in range(comps):
            field[k, n, plane(0)] = nothing
            field[k, n, plane(layers + 1)] = nothing

    for copy in scalars:
        copy.wait()
    column = lax.broadcasted_iota(jnp.int32, (around, lanes), 0)
    lane = lax.broadcasted_iota(jnp.int32, (around, lanes), 1)
    donor = jnp.zeros((around, lanes), jnp.int32)
    weight = jnp.zeros((around, lanes), jnp.float32)
    for j in range(around):
        donor = jnp.where(column == j, cells_ref[j], donor)
        weight = jnp.where(column == j, weights_ref[j], weight)
    for c in range(around + 1):
        blend[plane(c)] = jnp.where(donor == c, weight, 0.0) + jnp.where(donor + 1 == c, 1.0 - weight, 0.0)
    radial_lower = jnp.where(lane == 0, 0.0, LOWER).astype(jnp.float32)
    radial_upper = jnp.where(lane == lanes - 1, 0.0, UPPER).astype(jnp.float32)
    around_lower = jnp.where(column == 0, 0.0, LOWER).astype(jnp.float32)
    around_upper = jnp.where(column == around - 1, 0.0, UPPER).astype(jnp.float32)

    offset = offset_ref[0]
    chosen = []
    for step in range(lows):
        to = high * lows + partner(step)
        base = to + 2 * sectors - offset - 1
        ahead = lax.rem(low + lows - lax.rem(base, lows), lows)
        chosen.append(lax.rem(lax.div(base + ahead, lows), highs))
    slots = [lax.rem(low + 2 * sectors - offset - 1 + j, lows) for j in range(4)]

    into_field.wait()

    def slot_of(k):
        return (0, 2, 1)[k]

    def take_edges(k, sides=(0, 1)):
        for side in sides:
            for n in range(comps):
                edge[slot_of(k), side, item(n)] = field[k, n, column_of(rims[side], around)]

    take_edges(0)

    def remote(src, dst, send, recv, to):
        return pltpu.make_async_remote_copy(
            src_ref=src, dst_ref=dst, send_sem=send, recv_sem=recv, device_id=to, device_id_type=MESH
        )

    def beside(side):
        return (before if side else after, block)

    def edge_copy(k, side):
        i = slot_of(k)
        return remote(edge.at[i, side], halo.at[i, side], edge_send.at[i], edge_recv.at[i, side], beside(side))

    def part_copy(k, side):
        i = k // 2
        return remote(part.at[i, side], part_in.at[i, side], part_send.at[i], part_recv.at[i], beside(side))

    def coef_copy(side):
        return remote(coef.at[side], coef_in.at[side], coef_send, coef_recv, beside(side))

    def coef_pieces(side, pieces):
        for n in pieces:
            piece = pl.ds(n * comps * layers, comps * layers)
            remote(coef.at[side, piece], coef_in.at[side, piece], coef_send, coef_recv, beside(side)).start()

    def near_copy(side):
        return remote(near.at[side], near_in.at[side], near_send, near_recv, beside(side))

    def rim_copy(k, side):
        return remote(
            field.at[k, :, plane(1 if side else layers)],
            rim_in.at[k, side],
            rim_send.at[1 - side],
            rim_recv.at[k, 1 - side],
            (sector, block - 1 if side else block + 1),
        )

    def sent_rims(side):
        ours = rim_in.at[:, side]
        to = (sector, block - 1 if side else block + 1)
        return remote(ours, ours, rim_send.at[1 - side], rim_recv.at[0, 1 - side], to)

    def row_source(k):
        return row_out.at[k // 2] if k % 2 else field.at[k, :, plane(layers)]

    def row_copy(k, step):
        to = (high + step) % highs
        return remote(row_source(k), rows[k].at[high], row_send, row_recv.at[k], (to * lows + low, first))

    def all_rows(k):
        return remote(rows[k], rows[k], row_send, row_recv.at[k], (sector, first))

    def sent_rows():
        part = forward.at[:, pl.ds(0, highs)]
        return remote(part, part, row_send, row_recv.at[0], (sector, first))

    def cross_copy(step):
        to = (high + step) % highs
        return remote(cross_out, cross.at[high], cross_send, cross_recv, (to * lows + low, first))

    def all_crosses():
        return remote(cross, cross, cross_send, cross_recv, (sector, first))

    def forward_copy(k, step):
        to = (high * lows + partner(step), first)
        return remote(forward.at[k, step], picked[k].at[low], forward_send, forward_recv.at[k], to)

    def all_forwards(k):
        part = forward.at[k, pl.ds(1, lows - 1)]
        return remote(part, part, forward_send, forward_recv.at[k], (sector, first))

    def sent_forwards():
        part = forward.at[:, pl.ds(1, lows - 1)]
        return remote(part, part, forward_send, forward_recv.at[0], (sector, first))

    def cross_forward_copy(step):
        to = (high * lows + partner(step), first)
        return remote(
            cross_forward.at[step], cross_picked.at[low], cross_forward_send, cross_forward_recv, to
        )

    def all_cross_forwards():
        part = cross_forward.at[pl.ds(1, lows - 1)]
        return remote(part, part, cross_forward_send, cross_forward_recv, (sector, first))

    def both_edges(k):
        i = slot_of(k)
        return remote(edge.at[i], halo.at[i], edge_send.at[i], edge_recv.at[i, 0], beside(0))

    def both_parts(k):
        i = k // 2
        return remote(part.at[i], part_in.at[i], part_send.at[i], part_recv.at[i], beside(0))

    def both_near():
        return remote(near, near_in, near_send, near_recv, beside(0))

    near_last = sorted(range(lows), key=lambda step: -bin(step).count("1"))
    far_first = sorted(range(highs), key=lambda step: -min(step, highs - step))

    def send_rows(k):
        for step in far_first:
            row_copy(k, step).start()

    def send_rims(k):
        @pl.when(block > 0)
        def _():
            rim_copy(k, 1).start()

        @pl.when(has_upper)
        def _():
            rim_copy(k, 0).start()

    @pl.when(~is_end)
    def _():
        pl.semaphore_wait(barrier, greetings)

    send_rims(0)

    @pl.when(is_rotor_face)
    def _():
        send_rows(0)

    edge_copy(0, 0).start()

    @pl.when(~is_start)
    def _():
        edge_copy(0, 1).start()

    into_inverse.wait()

    def widen_inverse(i, carry):
        for m in range(comps):
            inverse[i, m] = inverse16[i, m].astype(jnp.float32).reshape(layers * around, lanes)
        return carry

    lax.fori_loop(0, comps, widen_inverse, 0)
    into_face.wait()

    def widen(i, carry):
        for d in range(3):
            for m in range(comps):
                face[d, i, m] = face16[d, i, m].astype(jnp.float32).reshape(layers * around, lanes)
        return carry

    lax.fori_loop(0, comps, widen, 0)

    def product(direction, where, share, store):
        inv = [[inverse[p, m, where] for m in range(comps)] for p in range(comps)]

        def body(n, carry):
            give = [share * face[direction, n, m, where] for m in range(comps)]
            for p in range(comps):
                total = inv[p][0] * give[0]
                for m in range(1, comps):
                    total = total + inv[p][m] * give[m]
                store(n * comps + p, total)
            return carry

        lax.fori_loop(0, comps, body, 0)

    for side in range(2):

        def keep(i, value):
            coef[side, pl.ds(pl.multiple_of(i * layers, layers), layers)] = value

        product(1, column_of(rims[side]), LOWER if side else UPPER, keep)

    @pl.when(is_rotor_face)
    def _():
        for side in range(2):
            for n in range(comps):
                cross_out[pl.ds(side * pairs + n * comps, comps)] = coef[
                    side, pl.ds(n * comps * layers + layers - 1, comps, stride=layers)
                ]
        for step in far_first:
            cross_copy(step).start()

    for side, (a, share) in enumerate(((0, LOWER), (layers - 1, UPPER))):

        def keep(i, value):
            axial[side, pl.ds(pl.multiple_of(i * around, around), around)] = value

        product(0, plane(a), share, keep)

    @pl.when(is_stator_face)
    def _():
        for side in range(2):
            for n in range(comps):
                near[side, pl.ds(comps + n * comps, comps)] = coef[side, pl.ds(n * comps * layers, comps, stride=layers)]
                near[side, pl.ds(comps + pairs + n * comps, comps)] = axial[
                    0, pl.ds(n * comps * around + rims[side], comps, stride=around)
                ]
            near[side, pl.ds(mixing, around)] = blend[pl.ds(rims[side], around, stride=around)]
            near[side, pl.ds(mixing + around, 1)] = blend[pl.ds(around * around + rims[side], 1)]

    into_source.wait()

    def make_radial(k):
        for n in range(comps):
            for a in range(layers):
                here = field[k, n, plane(a + 1)]
                radial[n, plane(a)] = radial_lower * pltpu.roll(here, 1, 1) + radial_upper * pltpu.roll(here, lanes - 1, 1)

    def local_part(k, a):
        acc = [source[m, plane(a)] for m in range(comps)]
        for n in range(comps):
            mix = radial[n, plane(a)]
            acc = [acc[m] + face[2, n, m, plane(a)] * mix for m in range(comps)]
        for n in range(comps):
            here = field[k, n, plane(a + 1)]
            mix = around_lower * pltpu.roll(here, 1, 0) + around_upper * pltpu.roll(here, around - 1, 0)
            acc = [acc[m] + face[1, n, m, plane(a)] * mix for m in range(comps)]
        for n in range(comps):
            mix = LOWER * field[k, n, plane(a)] + UPPER * field[k, n, plane(a + 2)]
            acc = [acc[m] + face[0, n, m, plane(a)] * mix for m in range(comps)]
        for m in range(comps):
            fresh = inverse[m, 0, plane(a)] * acc[0]
            for n in range(1, comps):
                fresh = fresh + inverse[m, n, plane(a)] * acc[n]
            if k < ITERS - 1:
                field[k + 1, m, plane(a + 1)] = fresh
            else:
                adjoint_ref[m, plane(a)] = 0.0 - fresh

    def send_part(k, side):
        for n in range(comps):
            part[k // 2, side, item(n)] = field[k + 1, n, column_of(rims[side], around)]
        part_copy(k, side).start()

    def local_parts(k, start, stop):
        def body(a, carry):
            local_part(k, a)
            return carry

        lax.fori_loop(start, stop, body, 0, unroll=UNROLL)

    def add_column(k, side, m, value, skip=0):
        if k < ITERS - 1:
            where = pl.ds((1 + skip) * around + rims[side], layers - skip, stride=around)
            value = value[skip:]
            field[k + 1, m, where] = field[k + 1, m, where] + value
        else:
            where = column_of(rims[side])
            adjoint_ref[m, where] = adjoint_ref[m, where] - value

    def add_plane(k, a, m, value):
        if k < ITERS - 1:
            field[k + 1, m, plane(a + 1)] = field[k + 1, m, plane(a + 1)] + value
        else:
            adjoint_ref[m, plane(a)] = adjoint_ref[m, plane(a)] - value

    def completed(k, s):
        i = k // 2
        own = [edge[i, 1 - s, item(n)] for n in range(comps)]
        values = []
        for m in range(comps):
            total = part_in[i, s, item(m)]
            for n in range(comps):
                total = total + coef_in[s, item(n * comps + m)] * own[n]
            values.append(total)
        return values

    def sent(k, s):
        return [part_in[k // 2, s, item(n)] for n in range(comps)]

    def received(k, s):
        return [halo[slot_of(k), s, item(n)] for n in range(comps)]

    def fix_side(k, side, halo_of, skip=0):
        given = halo_of(k, 1 - side)
        for m in range(comps):
            total = coef[side, item(m)] * given[0]
            for n in range(1, comps):
                total = total + coef[side, item(n * comps + m)] * given[n]
            add_column(k, side, m, total, skip)

    def by_place(body):
        for parity in range(2):

            @pl.when(sector % 2 == parity)
            def _():
                body(1 - parity, parity)

    def fix_layer(k, upper, given):
        a = layers - 1 if upper else 0
        for m in range(comps):
            total = axial[upper, plane(m)] * given[0]
            for n in range(1, comps):
                total = total + axial[upper, plane(n * comps + m)] * given[n]
            add_plane(k, a, m, total)

    def fix_upper(k):
        rim_copy(k, 1).wait_recv()
        fix_layer(k, 1, [rim_in[k, 1, n] for n in range(comps)])

    def fix_lower(k):
        rim_copy(k, 0).wait_recv()
        fix_layer(k, 0, [rim_in[k, 0, n] for n in range(comps)])

    def relay(k):
        all_rows(k).wait_recv()
        for step in near_last:
            if step:
                forward[k, step] = rows[k][chosen[step]]
                forward_copy(k, step).start()
            else:
                picked[k][low] = rows[k][chosen[step]]

    def relay_cross():
        all_crosses().wait_recv()
        for step in near_last:
            if step:
                cross_forward[step] = cross[chosen[step]]
                cross_forward_copy(step).start()
            else:
                cross_picked[low] = cross[chosen[step]]

    def got(k, j, n, c):
        return picked[k][slots[j], n, c : c + 1, :]

    def crossing(k):
        def one(j, side, other, c):
            total = None
            for n in range(comps):
                start = side * pairs + n * comps
                term = cross_picked[slots[j], start : start + comps, :] * got(k - 1, other, n, c)
                total = term if total is None else total + term
            return total

        return one(1, 1, 0, around - 1), one(1, 0, 2, 0), one(2, 1, 1, around - 1)

    def facing_of(k, extra):
        values = []
        for n in range(comps):
            total = blend[plane(around)] * got(k, 2, n, 0)
            for c in range(around):
                total = total + blend[plane(c)] * got(k, 1, n, c)
            if extra is not None:
                begin, end, next_begin = extra
                total = total + blend[plane(0)] * begin[n : n + 1] + blend[plane(around - 1)] * end[n : n + 1]
                total = total + blend[plane(around)] * next_begin[n : n + 1]
            values.append(total)
        return values

    def facing_beside(k, s):
        most, last = (0, 1) if s == 0 else (2, 3)
        ratios = near_in[s, pl.ds(mixing, around)]
        ratio = near_in[s, pl.ds(mixing + around, 1)]
        total = None
        for n in range(comps):
            value = jnp.sum(ratios * picked[k][slots[most], n], axis=0, keepdims=True) + ratio * got(k, last, n, 0)
            term = near_in[s, pl.ds(comps + pairs + n * comps, comps)] * value
            total = term if total is None else total + term
        return total

    def complete_parts(k):
        for s in range(2):
            where = pl.ds(0, comps, stride=layers)
            part_in[k // 2, s, where] = part_in[k // 2, s, where] + facing_beside(k, s)

    def complete_near():
        for s in range(2):
            total = near_in[s, pl.ds(0, comps)] + facing_beside(0, s)
            for n in range(comps):
                total = total + near_in[s, pl.ds(comps + n * comps, comps)] * edge[0, 1 - s, pl.ds(n * layers, 1)]
            near_halo[s] = total

    def fix_near():
        for side in range(2):
            total = None
            for n in range(comps):
                term = near[side, pl.ds(comps + n * comps, comps)] * near_halo[1 - side, pl.ds(n, 1)]
                total = term if total is None else total + term
            for m in range(comps):
                where = pl.ds(around + rims[side], 1)
                field[2, m, where] = field[2, m, where] + total[m : m + 1]

    def wait_forward(k):
        all_forwards(k).wait_recv()

    def wait_sends():
        coef_copy(0).wait_send()
        both_edges(0).wait_send()
        both_edges(2).wait_send()
        both_parts(2).wait_send()
        @pl.when(block > 0)
        def _():
            sent_rims(1).wait_send()

        @pl.when(has_upper)
        def _():
            sent_rims(0).wait_send()

        @pl.when(is_rotor_face)
        def _():
            all_crosses().wait_send()
            sent_rows().wait_send()

        @pl.when(is_stator_face)
        def _():
            both_near().wait_send()
            both_edges(1).wait_send()
            all_cross_forwards().wait_send()
            sent_forwards().wait_send()

        @pl.when(~is_stator_face)
        def _():
            edge_copy(1, 0).wait_send()
            part_copy(0, 0).wait_send()

    def arrive(k, side):
        edge_copy(k, 1 - side).wait_recv()

    for k in range(ITERS):
        last = k == ITERS - 1
        even = k % 2 == 0
        make_radial(k)
        local_parts(k, 0, layers)
        if last:
            for m in range(comps):
                update_ref[m] = field[k, m, pl.ds(around, layers * around)]

        @pl.when(has_lower)
        def _():
            fix_lower(k)

        if even:

            @pl.when(block < blocks - 1)
            def _():
                fix_upper(k)

            @pl.when(is_rotor_face)
            def _():
                for n in range(comps):
                    row_out[k // 2, n] = field[k + 1, n, plane(layers)]
                send_rows(k + 1)

            if k == 0:

                @pl.when(is_start)
                def _():
                    pl.semaphore_wait(ready, 1)
                    edge_copy(0, 1).start()

                @pl.when(is_stator_face)
                def _():
                    for side in range(2):
                        for m in range(comps):
                            near[side, pl.ds(m, 1)] = field[1, m, pl.ds(around + rims[side], 1)]
                        near_copy(side).start()

            def begin(far, close):
                if k == 0:

                    @pl.when(~is_stator_face)
                    def _():
                        send_part(0, far)
                        coef_pieces(far, range(comps))

                else:
                    send_part(k, far)
                arrive(k, close)
                fix_side(k, close, received)
                if k == 0:
                    take_edges(1, (close,))
                    edge_copy(1, close).start()
                else:
                    send_part(k, close)

                @pl.when(is_stator_face)
                def _():
                    relay(k)

                arrive(k, far)
                fix_side(k, far, received)
                if k == 0:

                    @pl.when(is_stator_face)
                    def _():
                        take_edges(1, (far,))
                        edge_copy(1, far).start()

            by_place(begin)

            @pl.when(is_stator_face)
            def _():
                if k == 0:
                    relay_cross()
                relay(k + 1)
                if k == 0:
                    by_place(lambda far, close: coef_pieces(far, range(0, 2)))
                    both_near().wait_recv()
                wait_forward(k)
                fix_layer(k, 0, facing_of(k, None))
                if k == 0:
                    by_place(lambda far, close: coef_pieces(far, range(2, 4)))

            send_rims(k + 1)
        elif not last:

            @pl.when(is_stator_face)
            def _():
                complete_near()
                fix_near()
                all_cross_forwards().wait_recv()
                extra = crossing(k)

                @pl.when(block < blocks - 1)
                def _():
                    fix_upper(k)

                wait_forward(k)
                fix_layer(k, 0, facing_of(k, extra))
                rim_copy(k + 1, 1).start()
                for side in range(2):
                    arrive(1, side)
                    fix_side(k, side, received, 1)

            @pl.when(~is_stator_face)
            def _():
                def finish(far, close):
                    arrive(1, close)
                    fix_side(k, close, received)
                    part_copy(0, 1 - far).wait_recv()
                    coef_copy(1 - far).wait_recv()
                    fix_side(k, far, completed)

                by_place(finish)

                @pl.when(block < blocks - 1)
                def _():
                    fix_upper(k)

                @pl.when(is_rotor_face)
                def _():
                    send_rows(k + 1)

                @pl.when(block > 0)
                def _():
                    rim_copy(k + 1, 1).start()

            @pl.when(has_upper)
            def _():
                rim_copy(k + 1, 0).start()

            take_edges(k + 1)

            def exchange(far, close):
                edge_copy(k + 1, far).start()
                edge_copy(k + 1, close).start()

                @pl.when(is_stator_face)
                def _():
                    coef_pieces(far, range(4, comps))

            by_place(exchange)
        else:
            both_parts(2).wait_recv()

            @pl.when(is_stator_face)
            def _():
                coef_copy(0).wait_recv()
                complete_parts(2)

            def end(far, close):
                fix_side(k, close, sent)
                fix_side(k, far, completed)

            by_place(end)
            wait_sends()

            @pl.when(block < blocks - 1)
            def _():
                fix_upper(k)

            @pl.when(is_stator_face)
            def _():
                extra = crossing(k)
                wait_forward(k)
                fix_layer(k, 0, facing_of(k, extra))


UNROLL = 2


def solution(mesh):
    sectors, blocks = mesh.shape["sector"], mesh.shape["block"]
    lows = low_part(sectors)
    highs = sectors // lows

    def sweeps(prev, source, face, inverse, offset, cells, weights):
        comps, layers, around, lanes = prev.shape
        f32, dma = jnp.float32, pltpu.SemaphoreType.DMA
        flat = (comps, layers * around, lanes)
        pairs = comps * comps
        row = (comps, around, lanes)
        cross = (2 * pairs, lanes)
        sides = (2, comps * layers, lanes)
        near = (2, comps + 2 * pairs + around + 1, lanes)
        hbm = pl.BlockSpec(memory_space=pl.ANY)
        vmem = pl.BlockSpec(memory_space=pltpu.VMEM)
        negative, previous = pl.pallas_call(
            functools.partial(kernel, sectors, blocks, layers, around),
            out_shape=(pltpu.VMEM(flat, f32),) * 2,
            in_specs=[hbm] * 7,
            out_specs=(vmem, vmem),
            scratch_shapes=[
                pltpu.SMEM(offset.shape, offset.dtype),
                pltpu.SMEM(cells.shape, cells.dtype),
                pltpu.SMEM(weights.shape, weights.dtype),
                pltpu.VMEM((ITERS, comps, (layers + 2) * around, lanes), f32),
                pltpu.VMEM(flat, f32),
                pltpu.VMEM(face.shape, face.dtype),
                pltpu.VMEM(inverse.shape, inverse.dtype),
                pltpu.VMEM((3, comps) + flat, f32),
                pltpu.VMEM((comps,) + flat, f32),
                pltpu.VMEM(flat, f32),
                pltpu.VMEM((3,) + sides, f32),
                pltpu.VMEM((3,) + sides, f32),
                pltpu.VMEM((2,) + sides, f32),
                pltpu.VMEM((2,) + sides, f32),
                pltpu.VMEM((2, pairs * layers, lanes), f32),
                pltpu.VMEM((2, pairs * layers, lanes), f32),
                pltpu.VMEM(near, f32),
                pltpu.VMEM(near, f32),
                pltpu.VMEM((2, comps, lanes), f32),
                pltpu.VMEM((2, pairs * around, lanes), f32),
                pltpu.VMEM((ITERS, 2) + row, f32),
                pltpu.VMEM((2,) + row, f32),
                [pltpu.VMEM((highs,) + row, f32)] * ITERS,
                pltpu.VMEM((ITERS, lows) + row, f32),
                [pltpu.VMEM((lows,) + row, f32)] * ITERS,
                pltpu.VMEM(cross, f32),
                pltpu.VMEM((highs,) + cross, f32),
                pltpu.VMEM((lows,) + cross, f32),
                pltpu.VMEM((lows,) + cross, f32),
                pltpu.VMEM(((around + 1) * around, lanes), f32),
                dma((7,)),
                pltpu.SemaphoreType.REGULAR,
                dma((3,)),
                dma((3, 2)),
                dma((2,)),
                dma((2,)),
                dma,
                dma,
                dma,
                dma,
                dma((min(blocks - 1, 2),)),
                dma((ITERS, min(blocks - 1, 2))),
                dma,
                dma((ITERS,)),
                dma,
                dma((ITERS,)),
                dma,
                dma,
                dma,
                dma,
            ],
            compiler_params=pltpu.CompilerParams(collective_id=0, has_side_effects=True),
        )(prev.reshape(flat), source.reshape(flat), face, inverse, offset, cells, weights)
        negative, previous = negative.reshape(prev.shape), previous.reshape(prev.shape)
        return 0.0 - negative, 0.0 - negative - previous

    return jax.shard_map(
        sweeps,
        mesh=mesh,
        in_specs=(
            P(None, "block", "sector", None),
            P(None, "block", "sector", None),
            P(None, None, None, "block", "sector", None),
            P(None, None, "block", "sector", None),
            P(),
            P("sector"),
            P("sector"),
        ),
        out_specs=(P(None, "block", "sector", None), P(None, "block", "sector", None)),
        check_vma=False,
    )
```
